256 devices in a mesh: seg: 4 (over y), sub: 64 (over z, x, core).
Axes of the slice: x: 4, y: 4, z: 8, core: 2. Of those that a mesh axis runs over, the one named last changes fastest.
Arguments:
- diffusivity: float32 [256, 32768], P('seg', 'sub'), may hold values from 0.01 to 0.4
- background_flow: float32 [256, 32768], P('seg', 'sub'), may hold values from 0.5 to 2
- inlet_modes: float32 [512, 32768], P(None, 'sub'), may hold values from -0.25 to 0.25
- profile_step: float32 [512], P('sub'), may hold values from -6 to 6
- brick_owner: int32 [65536, 1], P(('seg', 'sub')), may hold values from 0 to 63; in each aligned block of 256 rows (0 to 255, 256 to 511, ...) at most 8 rows name the same one
- voxel_row: int32 [65536], P(('seg', 'sub')), may hold values from 0 to 15
- noise_weight: float32 [4096, 128], P(('seg', 'sub')), may hold values from 0.1 to 10
- spread_matrix: float32 [128, 128], replicated, may hold values from -0.5 to 0.5
Outputs:
- forward_field: float32 [256, 32768], P('seg', 'sub')
- response: float32 [4096, 128], P(('seg', 'sub'))
- product: float32 [512], P(('seg', 'sub'))
The draws below stay inside these ranges and needn't reach their ends.
Inputs may be any that keep to these rules, and one draw needn't show every extreme that they name: `brick_owner`: among the 256 blocks of one device each brick index is named at most 8 times, and exactly 8 times on some device; blocks go to bricks of their own segment group.
All inputs are finite; a program needn't handle non-finite values.
Results may differ from the reference program's by a relative error of at most 0.00019.
Values sent between devices are 32-bit elements; how exact they have to be, the bound alone decides.
No kernel may reach another device: no remote copies, remote signals or barrier semaphores. Data moves between devices by JAX's collectives and lax.ppermute only.
A program may use at most 128 MiB of HBM per device.

```python
import math
import jax
import jax.numpy as jnp
import numpy as np
from jax import lax

AX = 64
CW = 512
BL = 128
VROWS = 16
NP = 512
NV = 2
SC = 2
NA = 256
NC = 32768
NB = 256
CAP = 8
BLOCKS = 65536
VOXROWS = 4096
N_SEG = 4
N_SUB = 64


def set_ends(entries, own_key, smallest, high):
    longest = entries.shape.index(max(entries.shape))
    spots = []
    for shift in (0, 1):
        where = [jax.random.randint(jax.random.fold_in(own_key, axis), (), 0, length) for axis, length in enumerate(entries.shape)]
        where[longest] = (where[longest] + shift) % entries.shape[longest]
        spots.append(tuple(where))
    return entries.at[spots[0]].set(smallest).at[spots[1]].set(high)


def block_levels(key, shape, cuts, least, top_value):
    factor_of = 1.0
    for axis_at, parts in cuts:
        steps = jax.random.uniform(jax.random.fold_in(jax.random.fold_in(key, 6), axis_at), (parts,), jnp.float32, least / len(cuts), top_value / len(cuts))
        factor_of = factor_of * jnp.repeat(jnp.exp(steps), shape[axis_at] // parts).reshape((-1,) + (1,) * (len(shape) - 1 - axis_at))
    return factor_of


def routed_block(rng, own, number, rows, amount, top, limit, slope):
    ranking = jax.random.permutation(rng, amount)
    crowded, ordinary = shares(amount, rows * top, limit, slope, True), shares(amount, rows * top, limit, slope, False)
    places = jnp.arange(amount)

    def named(tallies, turn):
        used = int((tallies > 0).sum())
        fixed = max(1, used // 4)
        moved = fixed + (places - fixed + turn * (used - fixed)) % max(1, amount - fixed)
        return jnp.zeros((amount,), jnp.int32).at[ranking[jnp.where(places < fixed, places, moved)]].set(jnp.asarray(tallies, jnp.int32))

    tallies = jnp.where(number % 4 == 0, named(crowded, number // 4), named(ordinary, number - number // 4 - 1))
    mixed = jax.random.permutation(jax.random.fold_in(own, 3), amount)
    giver, sink = mixed[0:amount // 2 * 2:2], mixed[1:amount // 2 * 2:2]
    slack = jnp.minimum(tallies[giver] - 1, limit - tallies[sink]) // 2
    slack = jnp.where((giver == ranking[0]) | (sink == ranking[0]) | (tallies[sink] == 0), 0, jnp.maximum(slack, 0))
    moved = jax.random.randint(jax.random.fold_in(own, 4), (amount // 2,), 0, 1 << 20) % (slack + 1)
    tallies = tallies.at[giver].add(-moved).at[sink].add(moved)
    labels = jnp.searchsorted(jnp.cumsum(tallies), jnp.arange(rows * top), side="right").astype(jnp.int32)
    grid = labels.reshape(top, rows).T
    grid = grid[jax.random.permutation(jax.random.fold_in(own, 1), rows)]
    turn = jax.random.randint(jax.random.fold_in(own, 2), (rows, 1), 0, top)
    return jnp.take_along_axis(grid, (jnp.arange(top)[None, :] + turn) % top, axis=1)


def shares(amount, total, bound, slope, full):
    weights = [(1 << 20) // math.isqrt(grade ** slope) + 1 for grade in range(1, amount + 1)]
    largest = bound if full else min(bound, max(-(-total // amount), total * weights[0] // sum(weights)))
    least = 1 if total - largest >= amount - 1 else 0
    holding, surplus = [largest] + [least] * (amount - 1), total - largest - least * (amount - 1)
    while surplus > 0:
        candidates = [i for i in range(1, amount) if holding[i] < largest] or [i for i in range(1, amount) if holding[i] < bound]
        pool, budget = sum([weights[i] for i in candidates]), surplus
        for i in candidates:
            extra = min(bound - holding[i], max(1, budget * weights[i] // pool), surplus)
            holding[i] = holding[i] + extra
            surplus = surplus - extra
    return np.array(holding)


def noise(rng, dims, width, reach, shards=(), held_as=jnp.bfloat16):
    drawn = width * jax.random.normal(rng, dims, jnp.float32)
    if shards:
        drawn = drawn * block_levels(rng, dims, shards, -0.22, 0.18)
    return jnp.clip(drawn, -reach, reach).astype(held_as)


def setup_inputs(seed: int = 0) -> dict:
    key_list = jax.random.split(jax.random.key(seed), 9)
    diffusivity = jnp.clip(jnp.exp(math.log(0.4) - 3.6888795 * jax.random.uniform(key_list[0], (NA, NC), jnp.float32) ** block_levels(key_list[0], (NA, NC), ((0, 4), (1, 64)), -0.2, 0.2)), 0.01, 0.4)
    background_flow = jnp.clip(jnp.exp(math.log(2.0) - 1.3862944 * jax.random.uniform(key_list[1], (NA, NC), jnp.float32) ** block_levels(key_list[1], (NA, NC), ((0, 4), (1, 64)), -0.2, 0.2)), 0.5, 2.0)
    inlet_modes = noise(key_list[2], (NP, NC), NP ** -0.5, 0.25, ((1, 64),), jnp.float32)
    profile_step = noise(key_list[3], (NP,), 1.0, 6.0, ((0, 64),), jnp.float32)
    brick_owner_keys = jax.random.split(jax.random.fold_in(key_list[4], 1), BLOCKS // NB)
    brick_owner_turns = jax.random.permutation(jax.random.fold_in(key_list[4], 3), BLOCKS // NB)
    brick_owner = jax.vmap(lambda own, number: routed_block(jax.random.fold_in(key_list[4], 2), own, number, NB, N_SUB, 1, CAP, 2))(brick_owner_keys, brick_owner_turns).reshape((BLOCKS, 1))
    voxel_row = set_ends(jax.random.randint(key_list[5], (BLOCKS,), 0, VROWS), jax.random.fold_in(key_list[5], 1), 0, VROWS - 1).astype(jnp.int32)
    noise_weight = jnp.clip(jnp.exp(math.log(10.0) - 4.6051702 * jax.random.uniform(key_list[6], (VOXROWS, BL), jnp.float32) ** block_levels(key_list[6], (VOXROWS, BL), ((0, 256),), -0.2, 0.2)), 0.1, 10.0)
    spread_matrix = noise(key_list[7], (BL, BL), BL ** -0.5, 0.5, (), jnp.float32)
    return {"diffusivity": diffusivity, "background_flow": background_flow, "inlet_modes": inlet_modes, "profile_step": profile_step, "brick_owner": brick_owner, "voxel_row": voxel_row, "noise_weight": noise_weight, "spread_matrix": spread_matrix}


SIGMA = 0.001
HIGH = lax.Precision.HIGHEST


def from_above(field):
    return jnp.pad(field, ((1, 0), (0, 0)))[:-1]


def from_below(field):
    return jnp.pad(field, ((0, 1), (0, 0)))[1:]


def from_left(field):
    return jnp.pad(field, ((0, 0), (1, 0)))[:, :-1]


def from_right(field):
    return jnp.pad(field, ((0, 0), (0, 1)))[:, 1:]


def make_stencil(diffusion, flow, reaction):
    return (4.0 * diffusion + flow + reaction, diffusion + flow, diffusion, diffusion, diffusion)


def transpose_stencil(stencil):
    diagonal, upstream, downstream, leftward, rightward = stencil
    return (diagonal, from_above(downstream), from_below(upstream), from_left(rightward), from_right(leftward))


def apply_operator(field, stencil):
    diagonal, upstream, downstream, leftward, rightward = stencil
    return (diagonal * field - upstream * from_above(field) - downstream * from_below(field)
            - leftward * from_left(field) - rightward * from_right(field))


def recurrence(gains, driving, reverse):
    def advance(carry, pieces):
        value = pieces[0] * carry + pieces[1]
        return value, value

    start_value = jnp.zeros(gains.shape[1], jnp.float32)
    _, values = lax.scan(advance, start_value, (gains, driving), reverse=reverse)
    return values


def relax(field, source, stencil, forward):
    diagonal, upstream, downstream, leftward, rightward = stencil
    lateral = leftward * from_left(field) + rightward * from_right(field)
    if forward:
        explicit = source + downstream * from_below(field) + lateral
        return recurrence(upstream / diagonal, explicit / diagonal, False)
    explicit = source + upstream * from_above(field) + lateral
    return recurrence(downstream / diagonal, explicit / diagonal, True)


def restrict(field):
    height, breadth = field.shape
    return field.reshape(height // 2, 2, breadth // 2, 2).sum(axis=(1, 3))


def aggregate(field):
    return restrict(field) * 0.25


def prolong(field):
    return jnp.repeat(jnp.repeat(field, 2, axis=0), 2, axis=1)


def vcycle(field, source, finest, coarse, forward):
    field = relax(field, source, finest, forward)
    coarse_source = restrict(source - apply_operator(field, finest))
    correction = jnp.zeros_like(coarse_source)
    for sweep_index in range(SC):
        correction = relax(correction, coarse_source, coarse, forward)
    field = field + prolong(correction)
    return relax(field, source, finest, forward)


def solve(source, finest, coarse, forward):
    field = jnp.zeros_like(source)
    for cycle_index in range(NV):
        field = vcycle(field, source, finest, coarse, forward)
    return field


def to_blocks(field):
    return field.reshape(N_SEG, AX, N_SUB, CW).transpose(0, 2, 1, 3).reshape(-1, BL)


def from_blocks(blocks):
    return blocks.reshape(N_SEG, N_SUB, AX, CW).transpose(0, 2, 1, 3).reshape(N_SEG * AX, N_SUB * CW)


def reference(diffusivity, background_flow, inlet_modes, profile_step, brick_owner, voxel_row, noise_weight, spread_matrix):
    finest = make_stencil(diffusivity, background_flow, SIGMA)
    coarse = make_stencil(aggregate(diffusivity), 2.0 * aggregate(background_flow), 4.0 * SIGMA)
    profile = jnp.dot(profile_step, inlet_modes, precision=HIGH)
    inflow = diffusivity[0] + background_flow[0]
    source = jnp.zeros_like(diffusivity).at[0].set(inflow * profile)
    forward_field = solve(source, finest, coarse, True)
    blocks = to_blocks(forward_field)
    segment = jnp.arange(blocks.shape[0], dtype=jnp.int32) // (N_SUB * NB)
    target = ((segment * N_SUB + brick_owner[:, 0]) * VROWS + voxel_row).astype(jnp.int32)
    voxels = jax.ops.segment_sum(blocks, target, num_segments=N_SEG * N_SUB * VROWS)
    response = jnp.dot(voxels, spread_matrix.T, precision=HIGH)
    weighted = jnp.dot(noise_weight * response, spread_matrix, precision=HIGH)
    driving = from_blocks(weighted[target])
    adjoint_field = solve(driving, transpose_stencil(finest), transpose_stencil(coarse), False)
    inlet_flux = inflow * adjoint_field[0]
    product = jnp.dot(inlet_modes, inlet_flux, precision=HIGH)
    return forward_field, response, product
```

```python
import jax
import jax.numpy as jnp
from jax import lax
from jax.experimental import pallas as pl
from jax.experimental.pallas import tpu as pltpu
from jax.sharding import PartitionSpec as P

SIGMA = 0.001
HIGH = lax.Precision.HIGHEST
BF = jnp.bfloat16
F32 = jnp.float32
HALO = 12
PAIRS = 76
T = 32
TC = 16
SLOTS = 8
VROWS = 16
ALL = ("seg", "sub")


def split3(x):
    hi = x.astype(BF)
    rest = x - hi.astype(F32)
    mid = rest.astype(BF)
    lo = (rest - mid.astype(F32)).astype(BF)
    return hi, mid, lo


def select_dot(x, chosen):
    hi, mid, lo = split3(x)
    out = jnp.dot(lo, chosen, preferred_element_type=F32)
    out = out + jnp.dot(mid, chosen, preferred_element_type=F32)
    return out + jnp.dot(hi, chosen, preferred_element_type=F32)


def lane(shape):
    return lax.broadcasted_iota(jnp.int32, shape, len(shape) - 1)


def sub(shape):
    return lax.broadcasted_iota(jnp.int32, shape, len(shape) - 2)


def to_pairs_matrix(offset):
    n = lane((256, 256))
    pair = jnp.where(n < 128, n, n - 128)
    x = 2 * pair + jnp.where(n < 128, 0, 1)
    source = jnp.where(
        x < HALO,
        128 + offset + x,
        jnp.where(x < HALO + 128, x - HALO, 128 + offset + x - 128),
    )
    hit = (source == sub((256, 256))) & (pair < PAIRS)
    return jnp.where(hit, 1.0, 0.0).astype(BF)


def from_pairs_matrix():
    row = sub((256, 128))
    y = lane((256, 128))
    source = (y >> 1) + HALO // 2 + jnp.where((y & 1) == 1, 128, 0)
    return jnp.where(source == row, 1.0, 0.0).astype(BF)


def edge_tile(tile_low, tile_high, shift):
    n = lane(tile_low.shape)
    base = shift - HALO
    low = jnp.where((n >= base) & (n < base + HALO), pltpu.roll(tile_low, shift, 1), 0.0)
    high = jnp.where(
        (n >= shift) & (n < shift + HALO), pltpu.roll(tile_high, shift, 1), 0.0
    )
    return low, high


def edges_kernel(k_ref, f_ref, up_ref, down_ref):
    kl, kh = edge_tile(k_ref[:, 384:512], k_ref[:, 0:128], HALO)
    fl, fh = edge_tile(f_ref[:, 384:512], f_ref[:, 0:128], 3 * HALO)
    up_ref[...] = kl + fl
    down_ref[...] = kh + fh


def spread_kernel(k_ref, f_ref, low_ref, high_ref, out_ref):
    for q in range(4):
        out_ref[q, 0] = k_ref[:, 128 * q : 128 * q + 128]
        out_ref[q, 1] = f_ref[:, 128 * q : 128 * q + 128]
        below = max(q - 1, 0)
        above = min(q + 1, 3)
        kl, kh = edge_tile(
            k_ref[:, 128 * below : 128 * below + 128],
            k_ref[:, 128 * above : 128 * above + 128],
            HALO,
        )
        fl, fh = edge_tile(
            f_ref[:, 128 * below : 128 * below + 128],
            f_ref[:, 128 * above : 128 * above + 128],
            3 * HALO,
        )
        low = low_ref[...] if q == 0 else kl + fl
        high = high_ref[...] if q == 3 else kh + fh
        out_ref[q, 2] = low + high


def profile_kernel(step_ref, modes_ref, out_ref):
    steps = step_ref[...]
    total = jnp.zeros((64, 128), F32)
    for j in range(8):
        total = total + steps[:, j : j + 1] * modes_ref[pl.ds(j, 64, stride=8), :]
    out_ref[0] = jnp.broadcast_to(jnp.sum(total, axis=0, keepdims=True), (8, 128))


def shifted(x, amount):
    n = sub(x.shape)
    if amount > 0:
        return jnp.where(n >= amount, pltpu.roll(x, amount, 0), 0.0)
    return jnp.where(n < 8 + amount, pltpu.roll(x, 8 + amount, 0), 0.0)


class Level:
    def __init__(self, gains, prefix, partial, count, forward):
        self.gains, self.prefix, self.partial = gains, prefix, partial
        self.count, self.forward = count, forward
        self.order = range(count) if forward else range(count - 1, -1, -1)

    def prepare(self, parts):
        one = 1 if self.forward else -1
        self.steps = []
        for p in range(parts):
            running = None
            for t in self.order:
                g = self.gains[p, t]
                running = g if running is None else running * g
                self.prefix[p, t] = running
            a = shifted(running, one)
            steps = []
            for d in (1, 2, 4):
                steps.append(a)
                a = a * shifted(a, one * d)
            self.steps.append(steps)

    def scan(self, parts, driving, emit):
        one = 1 if self.forward else -1
        running = [None] * parts
        for t in self.order:
            xs = driving(t)
            for p in range(parts):
                y = xs[p]
                if running[p] is not None:
                    y = self.gains[p, t] * running[p] + y
                running[p] = y
                self.partial[p, t] = y
        carry = []
        for p in range(parts):
            b = shifted(running[p], one)
            for d, a in zip((1, 2, 4), self.steps[p]):
                b = b + a * shifted(b, one * d)
            carry.append(b)
        for t in self.order:
            emit(t, [self.partial[p, t] + self.prefix[p, t] * carry[p] for p in range(parts)])


def beside(ref, t, count, forward, p):
    if forward:
        return ref[p, t + 1] if t + 1 < count else shifted(ref[p, 0], -1)
    return ref[p, t - 1] if t > 0 else shifted(ref[p, count - 1], 1)


def fine_sum(ref, t, forward):
    even, odd = ref[0, t], ref[1, t]
    return (
        beside(ref, t, T, forward, 0) + odd + pltpu.roll(odd, 1, 1),
        beside(ref, t, T, forward, 1) + even + pltpu.roll(even, 127, 1),
    )


def coarse_sum(ref, t, forward):
    own = ref[0, t]
    return beside(ref, t, TC, forward, 0) + pltpu.roll(own, 1, 1) + pltpu.roll(own, 127, 1)


SOLVE_SCRATCH = [
    pltpu.VMEM((2, T, 8, 128), F32),
    pltpu.VMEM((2, T, 8, 128), F32),
    pltpu.VMEM((2, T, 8, 128), F32),
    pltpu.VMEM((2, T, 8, 128), F32),
    pltpu.VMEM((2, T, 8, 128), F32),
    pltpu.VMEM((2, T, 8, 128), F32),
    pltpu.VMEM((1, TC, 8, 128), F32),
    pltpu.VMEM((1, TC, 8, 128), F32),
    pltpu.VMEM((1, TC, 8, 128), F32),
    pltpu.VMEM((1, TC, 8, 128), F32),
    pltpu.VMEM((1, TC, 8, 128), F32),
    pltpu.VMEM((1, TC, 8, 128), F32),
    pltpu.VMEM((1, TC, 8, 128), F32),
]


def solve_on_slab(kf, source, scratch, forward, finish):
    (gains, prefix, partial, scale, field, kept, cgains, cprefix, cpartial, cscale, ck, cfield,
     csource) = scratch
    for c in range(TC):
        ksum = fsum = None
        for t in (2 * c, 2 * c + 1):
            for p in range(2):
                k, f = kf[p, t], kf[2 + p, t]
                inverse = 1.0 / (4.0 * k + f + SIGMA)
                if forward:
                    gains[p, t] = (k + f) * inverse
                    scale[p, t] = k * inverse
                else:
                    if t + 1 < T:
                        up = kf[p, t + 1] + kf[2 + p, t + 1]
                    else:
                        up = shifted(kf[p, 0] + kf[2 + p, 0], -1)
                    gains[p, t] = up * inverse
                    scale[p, t] = inverse
                ksum = k if ksum is None else ksum + k
                fsum = f if fsum is None else fsum + f
        kc = 0.25 * ksum
        fc = 0.5 * fsum
        inverse = 1.0 / (4.0 * kc + fc + 4.0 * SIGMA)
        ck[0, c] = kc
        cfield[0, c] = kc + fc
        cscale[0, c] = inverse
    for c in range(TC):
        if forward:
            cgains[0, c] = cfield[0, c] * cscale[0, c]
        else:
            up = cfield[0, c + 1] if c + 1 < TC else shifted(cfield[0, 0], -1)
            cgains[0, c] = up * cscale[0, c]
    fine = Level(gains, prefix, partial, T, forward)
    fine.prepare(2)
    coarse = Level(cgains, cprefix, cpartial, TC, forward)
    coarse.prepare(1)

    def keep_fine(t, values):
        for p in range(2):
            field[p, t] = values[p] if forward else kf[p, t] * values[p]

    def correct(residual):
        for c in range(TC):
            total = None
            for t in (2 * c, 2 * c + 1):
                for part in residual(t):
                    total = part if total is None else total + part
            csource[0, c] = total * cscale[0, c]

        def keep_first(c, values):
            cfield[0, c] = values[0] if forward else ck[0, c] * values[0]

        coarse.scan(1, lambda c: (csource[0, c],), keep_first)

        def second(c):
            total = coarse_sum(cfield, c, forward)
            if forward:
                total = ck[0, c] * total
            return (csource[0, c] + cscale[0, c] * total,)

        def add_back(c, values):
            for t in (2 * c, 2 * c + 1):
                for p in range(2):
                    more = values[0] if forward else kf[p, t] * values[0]
                    field[p, t] = field[p, t] + more

        coarse.scan(1, second, add_back)

    def relaxed(t):
        sums = fine_sum(field, t, forward)
        start = source(t)
        return tuple(
            scale[p, t] * sums[p] if start is None else start[p] + scale[p, t] * sums[p]
            for p in range(2)
        )

    def started(t):
        start = source(t)
        return (jnp.zeros((8, 128), F32),) * 2 if start is None else start

    def residual_first(t):
        sums = fine_sum(field, t, forward)
        return tuple(kf[p, t] * sums[p] if forward else sums[p] for p in range(2))

    def relaxed_kept(t):
        sums = fine_sum(field, t, forward)
        start = source(t)
        for p in range(2):
            kept[p, t] = sums[p]
        return tuple(
            scale[p, t] * sums[p] if start is None else start[p] + scale[p, t] * sums[p]
            for p in range(2)
        )

    def residual_second(t):
        sums = fine_sum(field, t, forward)
        parts = tuple(sums[p] - kept[p, t] for p in range(2))
        return tuple(kf[p, t] * parts[p] if forward else parts[p] for p in range(2))

    fine.scan(2, started, keep_fine)
    correct(residual_first)
    fine.scan(2, relaxed, keep_fine)
    fine.scan(2, relaxed_kept, keep_fine)
    correct(residual_second)
    fine.scan(2, relaxed, finish)


def forward_kernel(place_ref, in_ref, own_ref, near_ref, out_ref, kf_ref, natural, *scratch):
    for field in range(2):
        chosen = to_pairs_matrix(2 * HALO * field)
        for g in range(4):
            x = jnp.concatenate([in_ref[g, field], in_ref[g, 2]], axis=1)
            got = select_dot(x, chosen)
            natural[0, 64 * g : 64 * g + 64] = got[:, :128]
            natural[1, 64 * g : 64 * g + 64] = got[:, 128:]
        for p in range(2):
            for t in range(T):
                kf_ref[2 * field + p, t] = natural[p, pl.ds(t, 8, stride=T), :]
    q = place_ref[0]
    low = jnp.where(q == 0, near_ref[3], own_ref[jnp.maximum(q - 1, 0)])
    high = jnp.where(q == 3, near_ref[0], own_ref[jnp.minimum(q + 1, 3)])
    parts = edge_tile(low, high, HALO)
    profile = select_dot(
        jnp.concatenate([own_ref[q], parts[0] + parts[1]], axis=1), to_pairs_matrix(0)
    )
    profile = jnp.where(sub((8, 256)) == 0, profile, 0.0)
    begin = []
    for p in range(2):
        k, f = kf_ref[p, 0], kf_ref[2 + p, 0]
        begin.append((k + f) * profile[:, 128 * p : 128 * p + 128] / (4.0 * k + f + SIGMA))
    result = scratch[2]

    def finish(t, values):
        for p in range(2):
            result[p, t] = values[p]

    solve_on_slab(kf_ref, lambda t: tuple(begin) if t == 0 else None, scratch, True, finish)
    chosen = from_pairs_matrix()
    both = jnp.concatenate(
        [result[0].reshape(256, 128), result[1].reshape(256, 128)], axis=1
    )
    got = select_dot(both, chosen)
    for t in range(T):
        out_ref[pl.ds(t, 8, stride=T), :] = got[8 * t : 8 * t + 8]


def pack_kernel(slot_ref, in_ref, field_ref, out_ref):
    for q in range(4):
        field_ref[:, 128 * q : 128 * q + 128] = in_ref[q]
    out_ref[...] = jnp.zeros(out_ref.shape, F32)
    for i in range(256):
        out_ref[pl.ds(slot_ref[i], 1), :] = in_ref[i // 64, i % 64 : i % 64 + 1]


def voxel_kernel(in_ref, row_ref, weight_ref, spread_ref, response_ref, out_ref):
    rows = jnp.broadcast_to(row_ref[...], (VROWS, 512))
    mask = jnp.where(rows == sub((VROWS, 512)).astype(F32), 1.0, 0.0)
    hi, mid, lo = split3(in_ref[...])
    chosen = mask.astype(BF)
    voxels = jnp.dot(chosen, lo, preferred_element_type=F32)
    voxels = voxels + jnp.dot(chosen, mid, preferred_element_type=F32)
    voxels = voxels + jnp.dot(chosen, hi, preferred_element_type=F32)
    spread = spread_ref[...]
    response = lax.dot_general(
        voxels, spread, (((1,), (1,)), ((), ())), precision=HIGH, preferred_element_type=F32
    )
    response_ref[...] = response
    weighted = jnp.dot(
        weight_ref[...] * response, spread, precision=HIGH, preferred_element_type=F32
    )
    back = jnp.transpose(mask).astype(BF)
    total = None
    for part in reversed(split3(weighted)):
        got = jnp.dot(back, part, preferred_element_type=F32)
        total = got if total is None else total + got
    out_ref[...] = total


def unpack_kernel(slot_ref, in_ref, out_ref, up_ref, down_ref):
    for i in range(256):
        out_ref[i // 64, i % 64 : i % 64 + 1] = in_ref[pl.ds(slot_ref[i], 1), :]
    low, high = edge_tile(out_ref[3], out_ref[0], HALO)
    up_ref[...] = low
    down_ref[...] = high


def driving_kernel(in_ref, low_ref, high_ref, out_ref):
    for q in range(4):
        out_ref[q, 0] = in_ref[q]
        low, high = edge_tile(in_ref[max(q - 1, 0)], in_ref[min(q + 1, 3)], HALO)
        if q == 0:
            low = low_ref[...]
        if q == 3:
            high = high_ref[...]
        out_ref[q, 1] = low + high


def adjoint_kernel(place_ref, in_ref, kf_ref, modes_ref, out_ref, natural, begin, *scratch):
    chosen = to_pairs_matrix(0)
    for g in range(4):
        x = jnp.concatenate([in_ref[g, 0], in_ref[g, 1]], axis=1)
        got = select_dot(x, chosen)
        natural[0, 64 * g : 64 * g + 64] = got[:, :128]
        natural[1, 64 * g : 64 * g + 64] = got[:, 128:]
    for p in range(2):
        for t in range(T):
            k, f = kf_ref[p, t], kf_ref[2 + p, t]
            begin[p, t] = natural[p, pl.ds(t, 8, stride=T), :] / (4.0 * k + f + SIGMA)
    flux = []

    def finish(t, values):
        if t == 0:
            for p in range(2):
                flux.append((kf_ref[p, 0] + kf_ref[2 + p, 0]) * values[p])

    solve_on_slab(kf_ref, lambda t: (begin[0, t], begin[1, t]), scratch, False, finish)
    natural_flux = select_dot(jnp.concatenate(flux, axis=1), from_pairs_matrix())
    row = natural_flux[0:1]
    out = jnp.zeros((256, 128), F32)
    for j in range(2):
        part = jnp.sum(modes_ref[pl.ds(j, 256, stride=2), :] * row, axis=1, keepdims=True)
        out = jnp.where(lane((256, 128)) == j, part, out)
    out_ref[...] = out


VM = pl.BlockSpec(memory_space=pltpu.VMEM)
SM = pl.BlockSpec(memory_space=pltpu.SMEM)


def shape(*dims):
    return jax.ShapeDtypeStruct(dims, F32)


def exchange(array, axis):
    return lax.all_to_all(array, axis, split_axis=0, concat_axis=0, tiled=True)


def on_device(
    diffusivity,
    background_flow,
    inlet_modes,
    profile_step,
    brick_owner,
    voxel_row,
    noise_weight,
    spread_matrix,
):
    count = lax.axis_size("sub")
    place = lax.axis_index("seg").astype(jnp.int32).reshape(1)
    up = [(i, i + 1) for i in range(count - 1)]
    down = [(i + 1, i) for i in range(count - 1)]

    to_up, to_down = pl.pallas_call(
        edges_kernel, out_shape=(shape(64, 128), shape(64, 128)), name="edges"
    )(diffusivity, background_flow)
    low = lax.ppermute(to_up, "sub", up)
    high = lax.ppermute(to_down, "sub", down)

    owners = brick_owner.reshape(64, 4).T.reshape(256)
    rows = voxel_row.reshape(64, 4).T.reshape(256)
    index = jnp.arange(256, dtype=jnp.int32)
    earlier = (owners[:, None] == owners[None, :]) & (index[:, None] < index[None, :])
    slots = owners * SLOTS + jnp.sum(earlier.astype(jnp.int32), axis=0)
    named = slots[:, None] == jnp.arange(count * SLOTS, dtype=jnp.int32)[None, :]
    slot_rows = VROWS - jnp.sum(jnp.where(named, VROWS - rows[:, None], 0), axis=0)
    message = jnp.concatenate(
        [
            jnp.broadcast_to(profile_step[None, :], (count, 8)),
            slot_rows.reshape(count, SLOTS).astype(F32),
            jnp.zeros((count, 112), F32),
        ],
        axis=1,
    )
    heard = exchange(message.reshape(count, 1, 128), "sub").reshape(count, 128)
    heard_rows = heard[:, 8:16].reshape(1, count * SLOTS)

    own_profile = pl.pallas_call(
        profile_kernel,
        grid=(4,),
        in_specs=[
            pl.BlockSpec((64, 128), lambda c: (0, 0)),
            pl.BlockSpec((512, 128), lambda c: (0, c)),
        ],
        out_specs=pl.BlockSpec((1, 8, 128), lambda c: (c, 0, 0)),
        out_shape=shape(4, 8, 128),
        name="profile",
    )(heard, inlet_modes)
    ends = [(i, i + 1) for i in range(count - 1)]
    ends += [(3 * count + i + 1, 3 * count + i) for i in range(count - 1)]
    near_profile = lax.ppermute(own_profile, ALL, ends)

    spread = pl.pallas_call(
        spread_kernel, out_shape=shape(4, 3, 64, 128), name="spread"
    )(diffusivity, background_flow, low, high)
    slab = exchange(spread, "seg")

    field, kf = pl.pallas_call(
        forward_kernel,
        in_specs=[SM, VM, VM, VM],
        out_shape=(shape(256, 128), shape(4, T, 8, 128)),
        scratch_shapes=[pltpu.VMEM((2, 256, 128), F32)] + SOLVE_SCRATCH,
        name="forward",
    )(place, slab, own_profile, near_profile)
    back = exchange(field.reshape(4, 64, 128), "seg")

    forward_field, packed = pl.pallas_call(
        pack_kernel,
        in_specs=[SM, VM],
        out_shape=(shape(64, 512), shape(count * SLOTS, 128)),
        name="pack",
    )(slots, back)
    arrived = exchange(packed.reshape(count, SLOTS, 128), "sub")

    response, answer = pl.pallas_call(
        voxel_kernel,
        out_shape=(shape(VROWS, 128), shape(count * SLOTS, 128)),
        name="voxels",
    )(arrived.reshape(count * SLOTS, 128), heard_rows, noise_weight, spread_matrix)
    answered = exchange(answer.reshape(count, SLOTS, 128), "sub")

    driving, to_up, to_down = pl.pallas_call(
        unpack_kernel,
        in_specs=[SM, VM],
        out_shape=(shape(4, 64, 128), shape(64, 128), shape(64, 128)),
        name="unpack",
    )(slots, answered.reshape(count * SLOTS, 128))
    low = lax.ppermute(to_up, "sub", up)
    high = lax.ppermute(to_down, "sub", down)
    spread = pl.pallas_call(
        driving_kernel, out_shape=shape(4, 2, 64, 128), name="driving"
    )(driving, low, high)
    slab = exchange(spread, "seg")

    partial = pl.pallas_call(
        adjoint_kernel,
        grid_spec=pltpu.PrefetchScalarGridSpec(
            num_scalar_prefetch=1,
            grid=(1,),
            in_specs=[
                pl.BlockSpec((4, 2, 64, 128), lambda i, q: (0, 0, 0, 0)),
                pl.BlockSpec((4, T, 8, 128), lambda i, q: (0, 0, 0, 0)),
                pl.BlockSpec((512, 128), lambda i, q: (0, q[0])),
            ],
            out_specs=pl.BlockSpec((256, 128), lambda i, q: (0, 0)),
            scratch_shapes=[
                pltpu.VMEM((2, 256, 128), F32),
                pltpu.VMEM((2, T, 8, 128), F32),
            ]
            + SOLVE_SCRATCH,
        ),
        out_shape=shape(256, 128),
        name="adjoint",
    )(place, slab, kf, inlet_modes)
    gathered = exchange(partial.reshape(256, 1, 128), ALL)
    product = jnp.sum(gathered, axis=(0, 1))[:2]
    return (forward_field, response, product)


def solution(mesh):
    in_specs = (
        P("seg", "sub"),
        P("seg", "sub"),
        P(None, "sub"),
        P("sub"),
        P(ALL, None),
        P(ALL),
        P(ALL, None),
        P(),
    )
    out_specs = (P("seg", "sub"), P(ALL, None), P(ALL))
    return jax.shard_map(
        on_device, mesh=mesh, in_specs=in_specs, out_specs=out_specs, check_vma=False
    )
```

```python
import jax
import jax.numpy as jnp
from jax import lax
from jax.experimental import pallas as pl
from jax.experimental.pallas import tpu as pltpu
from jax.sharding import PartitionSpec as P

SIGMA = 0.001
HIGH = lax.Precision.HIGHEST
BF = jnp.bfloat16
F32 = jnp.float32
HALO = 12
PAIRS = 76
T = 32
TC = 16
SLOTS = 8
VROWS = 16
ALL = ("seg", "sub")


def split3(x):
    hi = x.astype(BF)
    rest = x - hi.astype(F32)
    mid = rest.astype(BF)
    lo = (rest - mid.astype(F32)).astype(BF)
    return hi, mid, lo


def select_dot(x, chosen):
    hi, mid, lo = split3(x)
    out = jnp.dot(lo, chosen, preferred_element_type=F32)
    out = out + jnp.dot(mid, chosen, preferred_element_type=F32)
    return out + jnp.dot(hi, chosen, preferred_element_type=F32)


def lane(shape):
    return lax.broadcasted_iota(jnp.int32, shape, len(shape) - 1)


def sub(shape):
    return lax.broadcasted_iota(jnp.int32, shape, len(shape) - 2)


def to_pairs_matrix(offset):
    n = lane((256, 256))
    pair = jnp.where(n < 128, n, n - 128)
    x = 2 * pair + jnp.where(n < 128, 0, 1)
    source = jnp.where(
        x < HALO,
        128 + offset + x,
        jnp.where(x < HALO + 128, x - HALO, 128 + offset + x - 128),
    )
    hit = (source == sub((256, 256))) & (pair < PAIRS)
    return jnp.where(hit, 1.0, 0.0).astype(BF)


def from_pairs_matrix():
    row = sub((256, 128))
    y = lane((256, 128))
    source = (y >> 1) + HALO // 2 + jnp.where((y & 1) == 1, 128, 0)
    return jnp.where(source == row, 1.0, 0.0).astype(BF)


def edge_tile(tile_low, tile_high, shift):
    n = lane(tile_low.shape)
    base = shift - HALO
    low = jnp.where((n >= base) & (n < base + HALO), pltpu.roll(tile_low, shift, 1), 0.0)
    high = jnp.where(
        (n >= shift) & (n < shift + HALO), pltpu.roll(tile_high, shift, 1), 0.0
    )
    return low, high


def prepare_kernel(
    place_ref, k_ref, f_ref, owner_ref, row_ref, step_ref, *outs
):
    message_ref, slot_ref = outs[4:]
    owner_row = owner_ref[...]
    owner = jnp.transpose(jnp.broadcast_to(owner_row.astype(F32), (8, 256)))[:, 0:1]
    row = jnp.transpose(jnp.broadcast_to(row_ref[...].astype(F32), (8, 256)))[:, 0:1]
    same = owner == owner_row.astype(F32)
    i, j = sub((256, 256)), lane((256, 256))
    rank = jnp.sum(jnp.where(same & (j < i), 1.0, 0.0), axis=1, keepdims=True)
    rank_row = jnp.sum(jnp.where(same & (i < j), 1.0, 0.0), axis=0, keepdims=True)
    slots = owner_row * SLOTS + rank_row.astype(jnp.int32)
    slot_ref[...] = slots
    held = jnp.where(owner_row == sub((64, 256)), 1.0, 0.0).astype(BF)
    n = lane((256, 128))
    named = jnp.where(n == SLOTS + rank.astype(jnp.int32), row - float(VROWS), 0.0).astype(BF)
    n, m = lane((64, 128)), sub((64, 128))
    message = jnp.dot(held, named, preferred_element_type=F32) + jnp.where(
        (n >= SLOTS) & (n < 2 * SLOTS), float(VROWS), 0.0
    )
    spots = jnp.broadcast_to(slots.astype(F32), (8, 256))
    for q, towards in ((3, 1), (0, -1)):
        chosen = jnp.where(sub((256, 128)) == 4 * (lane((256, 128)) - 64) + q, 1.0, 0.0)
        told = select_dot(spots, chosen.astype(BF))[0:1]
        message = jnp.where((m == place_ref[1] + towards) & (n >= 64), told, message)
    message_ref[...] = message
    message_ref[:, 0:8] = jnp.broadcast_to(step_ref[...], (64, 8))
    for far in range(4):
        q = (place_ref[0] + far) & 3
        own = pl.ds(pl.multiple_of(128 * q, 128), 128)
        below = pl.ds(pl.multiple_of(128 * jnp.maximum(q - 1, 0), 128), 128)
        above = pl.ds(pl.multiple_of(128 * jnp.minimum(q + 1, 3), 128), 128)
        outs[far][0] = k_ref[:, own]
        outs[far][1] = f_ref[:, own]
        halo = jnp.zeros((64, 128), F32)
        for ref, shift in ((k_ref, HALO), (f_ref, 3 * HALO)):
            low, high = edge_tile(ref[:, below], ref[:, above], shift)
            halo = halo + jnp.where(q > 0, low, 0.0) + jnp.where(q < 3, high, 0.0)
        outs[far][2] = halo


def border_kernel(
    place_ref, heard_ref, modes_ref, slab_0, slab_1, slab_2, slab_3,
    profile_ref, slot_ref, out_ref, tile,
):
    q, u = place_ref[0], place_ref[1]
    heard = heard_ref[...]
    steps = [jnp.broadcast_to(heard[:, j : j + 1], (64, 128)) for j in range(8)]
    for c in range(4):
        tile[c] = modes_ref[:, 128 * c : 128 * c + 128]
        total = jnp.zeros((64, 128), F32)
        for j in range(8):
            total = total + steps[j] * tile[c, pl.ds(j, 64, stride=8), :]
        profile_ref[c] = jnp.broadcast_to(jnp.sum(total, axis=0, keepdims=True), (8, 128))
    m = sub((64, 128))
    for side, other in enumerate((u - 1, u + 1)):
        told = jnp.sum(jnp.where(m == other, heard, 0.0), axis=0, keepdims=True)
        slot_ref[side : side + 1] = pltpu.roll(told, 64, 1).astype(jnp.int32)
    n = lane((64, 128))
    sent = jnp.zeros((64, 128), F32)
    for far, slab_ref in enumerate((slab_0, slab_1, slab_2, slab_3)):
        k, f = slab_ref[0], slab_ref[1]
        k = jnp.where(n < HALO, jnp.where(q == 3, pltpu.roll(k, HALO, 1), k), 0.0)
        f = jnp.where(n < HALO, jnp.where(q == 3, pltpu.roll(f, HALO, 1), f), 0.0)
        both = k + pltpu.roll(f, HALO, 1)
        sent = sent + pltpu.roll(both, 2 * HALO * ((q - far) & 3), 1)
    out_ref[0:64] = sent
    out_ref[64:72] = jnp.where(q == 3, profile_ref[3], profile_ref[0])


def halo_from(near, g, first):
    n = lane((64, 128))
    x = pltpu.roll(near, (128 - 2 * HALO * g) & 127, 1)
    k = jnp.where(n < HALO, x, 0.0)
    f = jnp.where((n >= HALO) & (n < 2 * HALO), x, 0.0)
    low = k + pltpu.roll(f, HALO, 1)
    return jnp.where(first, low, pltpu.roll(low, HALO, 1))


def shifted(x, amount):
    n = sub(x.shape)
    if amount > 0:
        return jnp.where(n >= amount, pltpu.roll(x, amount, 0), 0.0)
    return jnp.where(n < 8 + amount, pltpu.roll(x, 8 + amount, 0), 0.0)


class Level:
    def __init__(self, gains, prefix, partial, count, forward):
        self.gains, self.prefix, self.partial = gains, prefix, partial
        self.count, self.forward = count, forward
        self.order = range(count) if forward else range(count - 1, -1, -1)

    def prepare(self, parts):
        one = 1 if self.forward else -1
        self.steps = []
        for p in range(parts):
            running = None
            for t in self.order:
                g = self.gains[p, t]
                running = g if running is None else running * g
                self.prefix[p, t] = running
            a = shifted(running, one)
            steps = []
            for d in (1, 2, 4):
                steps.append(a)
                a = a * shifted(a, one * d)
            self.steps.append(steps)

    def scan(self, parts, driving, emit):
        one = 1 if self.forward else -1
        running = [None] * parts
        for t in self.order:
            xs = driving(t)
            for p in range(parts):
                y = xs[p]
                if running[p] is not None:
                    y = self.gains[p, t] * running[p] + y
                running[p] = y
                self.partial[p, t] = y
        carry = []
        for p in range(parts):
            b = shifted(running[p], one)
            for d, a in zip((1, 2, 4), self.steps[p]):
                b = b + a * shifted(b, one * d)
            carry.append(b)
        for t in self.order:
            emit(t, [self.partial[p, t] + self.prefix[p, t] * carry[p] for p in range(parts)])


def beside(ref, t, count, forward, p):
    if forward:
        return ref[p, t + 1] if t + 1 < count else shifted(ref[p, 0], -1)
    return ref[p, t - 1] if t > 0 else shifted(ref[p, count - 1], 1)


def fine_sum(ref, t, forward):
    even, odd = ref[0, t], ref[1, t]
    return (
        beside(ref, t, T, forward, 0) + odd + pltpu.roll(odd, 1, 1),
        beside(ref, t, T, forward, 1) + even + pltpu.roll(even, 127, 1),
    )


def coarse_sum(ref, t, forward):
    own = ref[0, t]
    return beside(ref, t, TC, forward, 0) + pltpu.roll(own, 1, 1) + pltpu.roll(own, 127, 1)


SOLVE_SCRATCH = [
    pltpu.VMEM((2, T, 8, 128), F32),
    pltpu.VMEM((2, T, 8, 128), F32),
    pltpu.VMEM((2, T, 8, 128), F32),
    pltpu.VMEM((2, T, 8, 128), F32),
    pltpu.VMEM((2, T, 8, 128), F32),
    pltpu.VMEM((2, T, 8, 128), F32),
    pltpu.VMEM((1, TC, 8, 128), F32),
    pltpu.VMEM((1, TC, 8, 128), F32),
    pltpu.VMEM((1, TC, 8, 128), F32),
    pltpu.VMEM((1, TC, 8, 128), F32),
    pltpu.VMEM((1, TC, 8, 128), F32),
    pltpu.VMEM((1, TC, 8, 128), F32),
    pltpu.VMEM((1, TC, 8, 128), F32),
]


def solve_on_slab(kf, source, scratch, forward, finish):
    (gains, prefix, partial, scale, field, kept, cgains, cprefix, cpartial, cscale, ck, cfield,
     csource) = scratch
    for c in range(TC):
        ksum = fsum = None
        for t in (2 * c, 2 * c + 1):
            for p in range(2):
                k, f = kf[p, t], kf[2 + p, t]
                inverse = 1.0 / (4.0 * k + f + SIGMA)
                if forward:
                    gains[p, t] = (k + f) * inverse
                    scale[p, t] = k * inverse
                else:
                    if t + 1 < T:
                        up = kf[p, t + 1] + kf[2 + p, t + 1]
                    else:
                        up = shifted(kf[p, 0] + kf[2 + p, 0], -1)
                    gains[p, t] = up * inverse
                    scale[p, t] = inverse
                ksum = k if ksum is None else ksum + k
                fsum = f if fsum is None else fsum + f
        kc = 0.25 * ksum
        fc = 0.5 * fsum
        inverse = 1.0 / (4.0 * kc + fc + 4.0 * SIGMA)
        ck[0, c] = kc
        cfield[0, c] = kc + fc
        cscale[0, c] = inverse
    for c in range(TC):
        if forward:
            cgains[0, c] = cfield[0, c] * cscale[0, c]
        else:
            up = cfield[0, c + 1] if c + 1 < TC else shifted(cfield[0, 0], -1)
            cgains[0, c] = up * cscale[0, c]
    fine = Level(gains, prefix, partial, T, forward)
    fine.prepare(2)
    coarse = Level(cgains, cprefix, cpartial, TC, forward)
    coarse.prepare(1)

    def keep_fine(t, values):
        for p in range(2):
            field[p, t] = values[p] if forward else kf[p, t] * values[p]

    def correct(residual):
        for c in range(TC):
            total = None
            for t in (2 * c, 2 * c + 1):
                for part in residual(t):
                    total = part if total is None else total + part
            csource[0, c] = total * cscale[0, c]

        def keep_first(c, values):
            cfield[0, c] = values[0] if forward else ck[0, c] * values[0]

        coarse.scan(1, lambda c: (csource[0, c],), keep_first)

        def second(c):
            total = coarse_sum(cfield, c, forward)
            if forward:
                total = ck[0, c] * total
            return (csource[0, c] + cscale[0, c] * total,)

        def add_back(c, values):
            for t in (2 * c, 2 * c + 1):
                for p in range(2):
                    more = values[0] if forward else kf[p, t] * values[0]
                    field[p, t] = field[p, t] + more

        coarse.scan(1, second, add_back)

    def relaxed(t):
        sums = fine_sum(field, t, forward)
        start = source(t)
        return tuple(
            scale[p, t] * sums[p] if start is None else start[p] + scale[p, t] * sums[p]
            for p in range(2)
        )

    def started(t):
        start = source(t)
        return (jnp.zeros((8, 128), F32),) * 2 if start is None else start

    def residual_first(t):
        sums = fine_sum(field, t, forward)
        return tuple(kf[p, t] * sums[p] if forward else sums[p] for p in range(2))

    def relaxed_kept(t):
        sums = fine_sum(field, t, forward)
        start = source(t)
        for p in range(2):
            kept[p, t] = sums[p]
        return tuple(
            scale[p, t] * sums[p] if start is None else start[p] + scale[p, t] * sums[p]
            for p in range(2)
        )

    def residual_second(t):
        sums = fine_sum(field, t, forward)
        parts = tuple(sums[p] - kept[p, t] for p in range(2))
        return tuple(kf[p, t] * parts[p] if forward else parts[p] for p in range(2))

    fine.scan(2, started, keep_fine)
    correct(residual_first)
    fine.scan(2, relaxed, keep_fine)
    fine.scan(2, relaxed_kept, keep_fine)
    correct(residual_second)
    fine.scan(2, relaxed, finish)


def forward_kernel(
    place_ref, slab_0, slab_1, slab_2, slab_3, own_ref, near_ref, out_ref, kf_ref, natural, *scratch
):
    q = place_ref[0]
    outer = near_ref[0:64]
    chosen = [to_pairs_matrix(2 * HALO * field) for field in range(2)]
    for far, slab_ref in enumerate((slab_0, slab_1, slab_2, slab_3)):
        g = (q - far) & 3
        halo = slab_ref[2] + halo_from(outer, g, q == 0)
        rows = pl.ds(pl.multiple_of(64 * g, 64), 64)
        for field in range(2):
            x = jnp.concatenate([slab_ref[field], halo], axis=1)
            got = select_dot(x, chosen[field])
            natural[2 * field, rows, :] = got[:, :128]
            natural[2 * field + 1, rows, :] = got[:, 128:]
    for field in range(2):
        for p in range(2):
            for t in range(T):
                kf_ref[2 * field + p, t] = natural[2 * field + p, pl.ds(t, 8, stride=T), :]
    low = jnp.where(q == 0, near_ref[64:72], own_ref[jnp.maximum(q - 1, 0)])
    high = jnp.where(q == 3, near_ref[64:72], own_ref[jnp.minimum(q + 1, 3)])
    parts = edge_tile(low, high, HALO)
    profile = select_dot(
        jnp.concatenate([own_ref[q], parts[0] + parts[1]], axis=1), to_pairs_matrix(0)
    )
    profile = jnp.where(sub((8, 256)) == 0, profile, 0.0)
    begin = []
    for p in range(2):
        k, f = kf_ref[p, 0], kf_ref[2 + p, 0]
        begin.append((k + f) * profile[:, 128 * p : 128 * p + 128] / (4.0 * k + f + SIGMA))
    result = scratch[2]

    def finish(t, values):
        for p in range(2):
            result[p, t] = values[p]

    solve_on_slab(kf_ref, lambda t: tuple(begin) if t == 0 else None, scratch, True, finish)
    chosen = from_pairs_matrix()
    both = jnp.concatenate(
        [result[0].reshape(256, 128), result[1].reshape(256, 128)], axis=1
    )
    got = select_dot(both, chosen)
    for t in range(T):
        out_ref[pl.ds(t, 8, stride=T), :] = got[8 * t : 8 * t + 8]


def pack_kernel(slot_ref, in_ref, field_ref, out_ref):
    for q in range(4):
        field_ref[:, 128 * q : 128 * q + 128] = in_ref[q]
    out_ref[...] = jnp.zeros(out_ref.shape, F32)
    for i in range(256):
        r, q = divmod(i, 4)
        out_ref[pl.ds(slot_ref[i], 1), :] = in_ref[q, r : r + 1]


def voxel_kernel(in_ref, heard_ref, weight_ref, spread_ref, response_ref, out_ref):
    p = lane((128, 512))
    spot = jnp.where(sub((128, 512)) == SLOTS + (p & (SLOTS - 1)), 1.0, 0.0).astype(BF)
    rows = jnp.dot(heard_ref[...].astype(BF), spot, preferred_element_type=F32)
    mine = (lane((64, 512)) >> 3) == sub((64, 512))
    rows = jnp.sum(jnp.where(mine, rows, 0.0), axis=0, keepdims=True)
    rows = jnp.broadcast_to(rows, (VROWS, 512))
    mask = jnp.where(rows == sub((VROWS, 512)).astype(F32), 1.0, 0.0)
    chosen = mask.astype(BF)
    voxels = None
    for part in reversed(split3(in_ref[...])):
        got = jnp.dot(chosen, part, preferred_element_type=F32)
        voxels = got if voxels is None else voxels + got
    spread = spread_ref[...]
    response = lax.dot_general(
        voxels, spread, (((1,), (1,)), ((), ())), precision=HIGH, preferred_element_type=F32
    )
    response_ref[...] = response
    weighted = jnp.dot(
        weight_ref[...] * response, spread, precision=HIGH, preferred_element_type=F32
    )
    back = jnp.transpose(mask).astype(BF)
    total = None
    for part in reversed(split3(weighted)):
        got = jnp.dot(back, part, preferred_element_type=F32)
        total = got if total is None else total + got
    n = lane((8, 128))
    width = SLOTS + 2
    blank = jnp.zeros((1, 128), F32)
    out_ref[SLOTS] = blank
    out_ref[width * 63 + SLOTS + 1] = blank
    for u in range(64):
        own = total[SLOTS * u : SLOTS * u + SLOTS]
        for k in range(SLOTS):
            out_ref[width * u + k] = own[k : k + 1]
        if u < 63:
            last = jnp.where(n < HALO, pltpu.roll(own, HALO, 1), 0.0)
            last = pltpu.roll(last, 0, 1, stride=16, stride_axis=0)
            out_ref[width * (u + 1) + SLOTS] = jnp.sum(last, axis=0, keepdims=True)
        if u > 0:
            first = jnp.where(n < HALO, own, 0.0)
            first = pltpu.roll(first, 0, 1, stride=16, stride_axis=0)
            out_ref[width * (u - 1) + SLOTS + 1] = jnp.sum(first, axis=0, keepdims=True)


def driving_kernel(slot_ref, near_ref, in_ref, out_ref, ends):
    for i in range(256):
        r, q = divmod(i, 4)
        at = slot_ref[i]
        out_ref[q, 0, r : r + 1] = in_ref[at + 2 * (at >> 3)]
    for side in range(2):
        for r in range(64):
            at = near_ref[side, r]
            row = in_ref[(SLOTS + 2) * (at >> 3) + SLOTS + side]
            turn = (128 - 16 * (at & 7) + HALO * side) & 127
            ends[side, r : r + 1] = pltpu.roll(row, turn, 1)
    n = lane((64, 128))
    for q in range(4):
        low, high = edge_tile(out_ref[max(q - 1, 0), 0], out_ref[min(q + 1, 3), 0], HALO)
        if q == 0:
            low = jnp.where(n < HALO, ends[0], 0.0)
        if q == 3:
            high = jnp.where((n >= HALO) & (n < 2 * HALO), ends[1], 0.0)
        out_ref[q, 1] = low + high


def adjoint_kernel(place_ref, in_ref, kf_ref, modes_ref, out_ref, tile, natural, begin, *scratch):
    chosen = to_pairs_matrix(0)
    for g in range(4):
        x = jnp.concatenate([in_ref[g, 0], in_ref[g, 1]], axis=1)
        got = select_dot(x, chosen)
        natural[0, 64 * g : 64 * g + 64] = got[:, :128]
        natural[1, 64 * g : 64 * g + 64] = got[:, 128:]
    for p in range(2):
        for t in range(T):
            k, f = kf_ref[p, t], kf_ref[2 + p, t]
            begin[p, t] = natural[p, pl.ds(t, 8, stride=T), :] / (4.0 * k + f + SIGMA)
    flux = []

    def finish(t, values):
        if t == 0:
            for p in range(2):
                flux.append((kf_ref[p, 0] + kf_ref[2 + p, 0]) * values[p])

    solve_on_slab(kf_ref, lambda t: (begin[0, t], begin[1, t]), scratch, False, finish)
    natural_flux = select_dot(jnp.concatenate(flux, axis=1), from_pairs_matrix())
    row = natural_flux[0:1]
    out = jnp.zeros((256, 128), F32)
    column = pl.multiple_of(place_ref[0] * 128, 128)
    tile[...] = modes_ref[:, pl.ds(column, 128)]
    for j in range(2):
        modes = tile[pl.ds(j, 256, stride=2), :]
        part = jnp.sum(modes * row, axis=1, keepdims=True)
        out = jnp.where(lane((256, 128)) == j, part, out)
    out_ref[...] = out


VM = pl.BlockSpec(memory_space=pltpu.VMEM)
SM = pl.BlockSpec(memory_space=pltpu.SMEM)
PARAMS = pltpu.CompilerParams(vmem_limit_bytes=16 << 20)


def near(array):
    return pltpu.with_memory_space_constraint(array, pltpu.VMEM)


def held(*dims, dtype=F32):
    return pltpu.VMEM(dims, dtype)


def run(kernel, name, ins, outs, scratch=(), pinned=True):
    scalars = [array.dtype == jnp.int32 and name != "prepare" for array in ins]
    scalars[0] = ins[0].dtype == jnp.int32
    specs = [SM if scalar else VM if pinned else pl.BlockSpec() for scalar in scalars]
    if pinned:
        ins = [array if scalar else near(array) for array, scalar in zip(ins, scalars)]
    else:
        ins = [array if scalar else pltpu.with_memory_space_constraint(array, pltpu.HBM)
               for array, scalar in zip(ins, scalars)]
    return pl.pallas_call(
        kernel,
        in_specs=specs,
        out_specs=[VM] * len(outs),
        out_shape=outs,
        scratch_shapes=list(scratch),
        compiler_params=PARAMS,
        name=name,
    )(*ins)


def exchange(array, axis):
    return lax.all_to_all(array, axis, split_axis=0, concat_axis=0, tiled=True)


def on_device(
    diffusivity,
    background_flow,
    inlet_modes,
    profile_step,
    brick_owner,
    voxel_row,
    noise_weight,
    spread_matrix,
):
    count = lax.axis_size("sub")
    place = jnp.stack([lax.axis_index("seg"), lax.axis_index("sub")]).astype(jnp.int32)

    *slab, message, slots = run(
        prepare_kernel,
        "prepare",
        (
            place,
            diffusivity,
            background_flow,
            brick_owner.reshape(1, 256),
            voxel_row.reshape(1, 256),
            profile_step.reshape(1, 8),
        ),
        (held(3, 64, 128),) * 4 + (held(64, 128), held(1, 256, dtype=jnp.int32)),
        pinned=False,
    )
    slots = slots.reshape(256)
    for far in (2, 1, 3):
        slab[far] = lax.ppermute(slab[far], "seg", [(i, (i + far) % 4) for i in range(4)])
    heard = exchange(message.reshape(count, 1, 128), "sub").reshape(count, 128)

    own_profile, near_slots, to_near = run(
        border_kernel,
        "border",
        (place, heard, inlet_modes, *slab),
        (held(4, 8, 128), held(2, 128, dtype=jnp.int32), held(72, 128)),
        [pltpu.VMEM((4, 512, 128), F32)],
    )
    outward = [(3 * count + i, i + 1) for i in range(count - 1)]
    outward += [(i + 1, 3 * count + i) for i in range(count - 1)]
    from_near = lax.ppermute(to_near, ALL, outward)

    field, kf = run(
        forward_kernel,
        "forward",
        (place, *slab, own_profile, from_near),
        (held(256, 128), held(4, T, 8, 128)),
        [pltpu.VMEM((4, 256, 128), F32)] + SOLVE_SCRATCH,
    )
    back = exchange(field.reshape(4, 64, 128), "seg")

    forward_field, packed = run(
        pack_kernel, "pack", (slots, back), (held(64, 512), held(count * SLOTS, 128))
    )
    arrived = exchange(packed.reshape(count, SLOTS, 128), "sub")

    response, answer = run(
        voxel_kernel,
        "voxels",
        (arrived.reshape(count * SLOTS, 128), heard, noise_weight, spread_matrix),
        (held(VROWS, 128), held(count * (SLOTS + 2), 1, 128)),
    )
    answered = exchange(answer, "sub")

    (spread,) = run(
        driving_kernel,
        "driving",
        (slots, near_slots, answered),
        (held(4, 2, 64, 128),),
        [pltpu.VMEM((2, 64, 128), F32)],
    )
    slab = exchange(spread, "seg")

    (partial,) = run(
        adjoint_kernel,
        "adjoint",
        (place, slab, kf, inlet_modes),
        (held(256, 128),),
        [
            pltpu.VMEM((512, 128), F32),
            pltpu.VMEM((2, 256, 128), F32),
            pltpu.VMEM((2, T, 8, 128), F32),
        ]
        + SOLVE_SCRATCH,
    )
    gathered = exchange(partial.reshape(256, 1, 128), ALL)
    product = jnp.sum(gathered, axis=(0, 1))[:2]
    return (forward_field, response, product)


def solution(mesh):
    in_specs = (
        P("seg", "sub"),
        P("seg", "sub"),
        P(None, "sub"),
        P("sub"),
        P(ALL, None),
        P(ALL),
        P(ALL, None),
        P(),
    )
    out_specs = (P("seg", "sub"), P(ALL, None), P(ALL))
    return jax.shard_map(
        on_device, mesh=mesh, in_specs=in_specs, out_specs=out_specs, check_vma=False
    )
```

```python
import jax
import jax.numpy as jnp
from jax import lax
from jax.experimental import pallas as pl
from jax.experimental.pallas import tpu as pltpu
from jax.sharding import PartitionSpec as P

SIGMA = 0.001
HIGH = lax.Precision.HIGHEST
BF = jnp.bfloat16
F32 = jnp.float32
HALO = 12
PAIRS = 76
T = 32
TC = 16
SLOTS = 8
VROWS = 16
ALL = ("seg", "sub")


def split3(x):
    hi = x.astype(BF)
    rest = x - hi.astype(F32)
    mid = rest.astype(BF)
    lo = (rest - mid.astype(F32)).astype(BF)
    return hi, mid, lo


def select_dot(x, chosen):
    hi, mid, lo = split3(x)
    out = jnp.dot(lo, chosen, preferred_element_type=F32)
    out = out + jnp.dot(mid, chosen, preferred_element_type=F32)
    return out + jnp.dot(hi, chosen, preferred_element_type=F32)


def lane(shape):
    return lax.broadcasted_iota(jnp.int32, shape, len(shape) - 1)


def sub(shape):
    return lax.broadcasted_iota(jnp.int32, shape, len(shape) - 2)


def to_pairs_matrix(offset):
    n = lane((256, 256))
    pair = jnp.where(n < 128, n, n - 128)
    x = 2 * pair + jnp.where(n < 128, 0, 1)
    source = jnp.where(
        x < HALO,
        128 + offset + x,
        jnp.where(x < HALO + 128, x - HALO, 128 + offset + x - 128),
    )
    hit = (source == sub((256, 256))) & (pair < PAIRS)
    return jnp.where(hit, 1.0, 0.0).astype(BF)


def from_pairs_matrix():
    row = sub((256, 128))
    y = lane((256, 128))
    source = (y >> 1) + HALO // 2 + jnp.where((y & 1) == 1, 128, 0)
    return jnp.where(source == row, 1.0, 0.0).astype(BF)


def edge_tile(tile_low, tile_high, shift):
    n = lane(tile_low.shape)
    base = shift - HALO
    low = jnp.where((n >= base) & (n < base + HALO), pltpu.roll(tile_low, shift, 1), 0.0)
    high = jnp.where(
        (n >= shift) & (n < shift + HALO), pltpu.roll(tile_high, shift, 1), 0.0
    )
    return low, high


def prepare_kernel(
    place_ref, k_ref, f_ref, owner_ref, row_ref, step_ref, modes_ref, *outs
):
    message_ref, slot_ref, tile, sems = outs[4:]
    copies = []
    for i in range(3):
        start = 128 * jnp.clip(place_ref[0] + i - 1, 0, 3)
        copies.append(
            pltpu.make_async_copy(
                modes_ref.at[:, pl.ds(pl.multiple_of(start, 128), 128)], tile.at[i], sems.at[i]
            )
        )
        copies[-1].start()
    owner_row = owner_ref[...]
    owner = jnp.transpose(jnp.broadcast_to(owner_row.astype(F32), (8, 256)))[:, 0:1]
    row = jnp.transpose(jnp.broadcast_to(row_ref[...].astype(F32), (8, 256)))[:, 0:1]
    same = owner == owner_row.astype(F32)
    i, j = sub((256, 256)), lane((256, 256))
    rank = jnp.sum(jnp.where(same & (j < i), 1.0, 0.0), axis=1, keepdims=True)
    rank_row = jnp.sum(jnp.where(same & (i < j), 1.0, 0.0), axis=0, keepdims=True)
    slots = owner_row * SLOTS + rank_row.astype(jnp.int32)
    slot_ref[...] = slots
    held = jnp.where(owner_row == sub((64, 256)), 1.0, 0.0).astype(BF)
    n = lane((256, 128))
    named = jnp.where(n == SLOTS + rank.astype(jnp.int32), row - float(VROWS), 0.0).astype(BF)
    n, m = lane((64, 128)), sub((64, 128))
    message = jnp.dot(held, named, preferred_element_type=F32) + jnp.where(
        (n >= SLOTS) & (n < 2 * SLOTS), float(VROWS), 0.0
    )
    spots = jnp.broadcast_to(slots.astype(F32), (8, 256))
    for q, towards in ((3, 1), (0, -1)):
        chosen = jnp.where(sub((256, 128)) == 4 * (lane((256, 128)) - 64) + q, 1.0, 0.0)
        told = select_dot(spots, chosen.astype(BF))[0:1]
        message = jnp.where((m == place_ref[1] + towards) & (n >= 64), told, message)
    message_ref[...] = message
    message_ref[:, 0:8] = jnp.broadcast_to(step_ref[...], (64, 8))
    for far in range(4):
        q = (place_ref[0] + far) & 3
        own = pl.ds(pl.multiple_of(128 * q, 128), 128)
        below = pl.ds(pl.multiple_of(128 * jnp.maximum(q - 1, 0), 128), 128)
        above = pl.ds(pl.multiple_of(128 * jnp.minimum(q + 1, 3), 128), 128)
        outs[far][0] = k_ref[:, own]
        outs[far][1] = f_ref[:, own]
        halo = jnp.zeros((64, 128), F32)
        for ref, shift in ((k_ref, HALO), (f_ref, 3 * HALO)):
            low, high = edge_tile(ref[:, below], ref[:, above], shift)
            halo = halo + jnp.where(q > 0, low, 0.0) + jnp.where(q < 3, high, 0.0)
        outs[far][2] = halo
    for copy in copies:
        copy.wait()


def border_kernel(
    place_ref, tile, message_ref, slab_0, slab_1, slab_2, slab_3, out_ref, told_ref
):
    q = place_ref[0]
    told_ref[...] = message_ref[...]
    n = lane((64, 128))
    sent = jnp.zeros((64, 128), F32)
    for far, slab_ref in enumerate((slab_0, slab_1, slab_2, slab_3)):
        k, f = slab_ref[0], slab_ref[1]
        k = jnp.where(n < HALO, jnp.where(q == 3, pltpu.roll(k, HALO, 1), k), 0.0)
        f = jnp.where(n < HALO, jnp.where(q == 3, pltpu.roll(f, HALO, 1), f), 0.0)
        both = k + pltpu.roll(f, HALO, 1)
        sent = sent + pltpu.roll(both, 2 * HALO * ((q - far) & 3), 1)
    out_ref[0:64] = sent
    sent = jnp.zeros((64, 128), F32)
    for j in range(8):
        x = tile[1, pl.ds(j, 64, stride=8), :]
        x = jnp.where(n < HALO, jnp.where(q == 3, pltpu.roll(x, HALO, 1), x), 0.0)
        sent = sent + (pltpu.roll(x, 16 * j, 1) if j else x)
    out_ref[64:128] = sent


def halo_from(near, g, first):
    n = lane((64, 128))
    x = pltpu.roll(near, (128 - 2 * HALO * g) & 127, 1)
    k = jnp.where(n < HALO, x, 0.0)
    f = jnp.where((n >= HALO) & (n < 2 * HALO), x, 0.0)
    low = k + pltpu.roll(f, HALO, 1)
    return jnp.where(first, low, pltpu.roll(low, HALO, 1))


def shifted(x, amount):
    n = sub(x.shape)
    if amount > 0:
        return jnp.where(n >= amount, pltpu.roll(x, amount, 0), 0.0)
    return jnp.where(n < 8 + amount, pltpu.roll(x, 8 + amount, 0), 0.0)


class Level:
    def __init__(self, gains, prefix, partial, count, forward):
        self.gains, self.prefix, self.partial = gains, prefix, partial
        self.count, self.forward = count, forward
        self.order = range(count) if forward else range(count - 1, -1, -1)

    def multiply(self, parts):
        for p in range(parts):
            running = None
            for t in self.order:
                g = self.gains[p, t]
                running = g if running is None else running * g
                self.prefix[p, t] = running

    def prepare(self, parts):
        one = 1 if self.forward else -1
        self.steps = []
        for p in range(parts):
            a = shifted(self.prefix[p, self.order[-1]], one)
            steps = []
            for d in (1, 2, 4):
                steps.append(a)
                a = a * shifted(a, one * d)
            self.steps.append(steps)

    def scan(self, parts, driving, emit):
        one = 1 if self.forward else -1
        running = [None] * parts
        for t in self.order:
            xs = driving(t)
            for p in range(parts):
                y = xs[p]
                if running[p] is not None:
                    y = self.gains[p, t] * running[p] + y
                running[p] = y
                self.partial[p, t] = y
        carry = []
        for p in range(parts):
            b = shifted(running[p], one)
            for d, a in zip((1, 2, 4), self.steps[p]):
                b = b + a * shifted(b, one * d)
            carry.append(b)
        for t in self.order:
            emit(t, [self.partial[p, t] + self.prefix[p, t] * carry[p] for p in range(parts)])


def beside(ref, t, count, forward, p):
    if forward:
        return ref[p, t + 1] if t + 1 < count else shifted(ref[p, 0], -1)
    return ref[p, t - 1] if t > 0 else shifted(ref[p, count - 1], 1)


def fine_sum(ref, t, forward):
    even, odd = ref[0, t], ref[1, t]
    return (
        beside(ref, t, T, forward, 0) + odd + pltpu.roll(odd, 1, 1),
        beside(ref, t, T, forward, 1) + even + pltpu.roll(even, 127, 1),
    )


def coarse_sum(ref, t, forward):
    own = ref[0, t]
    return beside(ref, t, TC, forward, 0) + pltpu.roll(own, 1, 1) + pltpu.roll(own, 127, 1)


STENCIL_SHAPES = [(2, T, 8, 128)] * 3 + [(1, TC, 8, 128)] * 4
WORK_SHAPES = [(2, T, 8, 128)] * 3 + [(1, TC, 8, 128)] * 3
SOLVE_SCRATCH = [pltpu.VMEM(dims, F32) for dims in STENCIL_SHAPES + WORK_SHAPES]


def build_stencils(kf, stencils, sums, forward):
    gains, prefix, scale, cgains, cprefix, cscale, ck = stencils
    for c in range(TC):
        ksum = fsum = None
        for t in (2 * c, 2 * c + 1):
            for p in range(2):
                k, f = kf[p, t], kf[2 + p, t]
                inverse = 1.0 / (4.0 * k + f + SIGMA)
                if forward:
                    gains[p, t] = (k + f) * inverse
                    scale[p, t] = k * inverse
                else:
                    if t + 1 < T:
                        up = kf[p, t + 1] + kf[2 + p, t + 1]
                    else:
                        up = shifted(kf[p, 0] + kf[2 + p, 0], -1)
                    gains[p, t] = up * inverse
                    scale[p, t] = inverse
                ksum = k if ksum is None else ksum + k
                fsum = f if fsum is None else fsum + f
        kc = 0.25 * ksum
        fc = 0.5 * fsum
        inverse = 1.0 / (4.0 * kc + fc + 4.0 * SIGMA)
        ck[0, c] = kc
        sums[0, c] = kc + fc
        cscale[0, c] = inverse
    for c in range(TC):
        if forward:
            cgains[0, c] = sums[0, c] * cscale[0, c]
        else:
            up = sums[0, c + 1] if c + 1 < TC else shifted(sums[0, 0], -1)
            cgains[0, c] = up * cscale[0, c]
    Level(gains, prefix, None, T, forward).multiply(2)
    Level(cgains, cprefix, None, TC, forward).multiply(1)


def solve_on_slab(kf, source, stencils, work, forward, finish):
    gains, prefix, scale, cgains, cprefix, cscale, ck = stencils
    partial, field, kept, cpartial, cfield, csource = work
    fine = Level(gains, prefix, partial, T, forward)
    fine.prepare(2)
    coarse = Level(cgains, cprefix, cpartial, TC, forward)
    coarse.prepare(1)

    def keep_fine(t, values):
        for p in range(2):
            field[p, t] = values[p] if forward else kf[p, t] * values[p]

    def correct(residual):
        for c in range(TC):
            total = None
            for t in (2 * c, 2 * c + 1):
                for part in residual(t):
                    total = part if total is None else total + part
            csource[0, c] = total * cscale[0, c]

        def keep_first(c, values):
            cfield[0, c] = values[0] if forward else ck[0, c] * values[0]

        coarse.scan(1, lambda c: (csource[0, c],), keep_first)

        def second(c):
            total = coarse_sum(cfield, c, forward)
            if forward:
                total = ck[0, c] * total
            return (csource[0, c] + cscale[0, c] * total,)

        def add_back(c, values):
            for t in (2 * c, 2 * c + 1):
                for p in range(2):
                    more = values[0] if forward else kf[p, t] * values[0]
                    field[p, t] = field[p, t] + more

        coarse.scan(1, second, add_back)

    def relaxed(t):
        sums = fine_sum(field, t, forward)
        start = source(t)
        return tuple(
            scale[p, t] * sums[p] if start is None else start[p] + scale[p, t] * sums[p]
            for p in range(2)
        )

    def started(t):
        start = source(t)
        return (jnp.zeros((8, 128), F32),) * 2 if start is None else start

    def residual_first(t):
        sums = fine_sum(field, t, forward)
        return tuple(kf[p, t] * sums[p] if forward else sums[p] for p in range(2))

    def relaxed_kept(t):
        sums = fine_sum(field, t, forward)
        start = source(t)
        for p in range(2):
            kept[p, t] = sums[p]
        return tuple(
            scale[p, t] * sums[p] if start is None else start[p] + scale[p, t] * sums[p]
            for p in range(2)
        )

    def residual_second(t):
        sums = fine_sum(field, t, forward)
        parts = tuple(sums[p] - kept[p, t] for p in range(2))
        return tuple(kf[p, t] * parts[p] if forward else parts[p] for p in range(2))

    fine.scan(2, started, keep_fine)
    correct(residual_first)
    fine.scan(2, relaxed, keep_fine)
    fine.scan(2, relaxed_kept, keep_fine)
    correct(residual_second)
    fine.scan(2, relaxed, finish)


def forward_kernel(
    place_ref, slab_0, slab_1, slab_2, slab_3, near_ref, heard_ref, tile,
    out_ref, kf_ref, slot_ref, natural, *scratch,
):
    heard = heard_ref[...]
    for side, other in enumerate((place_ref[1] - 1, place_ref[1] + 1)):
        told = jnp.sum(jnp.where(sub((64, 128)) == other, heard, 0.0), axis=0, keepdims=True)
        slot_ref[side : side + 1] = pltpu.roll(told, 64, 1).astype(jnp.int32)
    q = place_ref[0]
    outer = near_ref[0:64]
    chosen = [to_pairs_matrix(2 * HALO * field) for field in range(2)]
    for far, slab_ref in enumerate((slab_0, slab_1, slab_2, slab_3)):
        g = (q - far) & 3
        halo = slab_ref[2] + halo_from(outer, g, q == 0)
        rows = pl.ds(pl.multiple_of(64 * g, 64), 64)
        for field in range(2):
            x = jnp.concatenate([slab_ref[field], halo], axis=1)
            got = select_dot(x, chosen[field])
            natural[2 * field, rows, :] = got[:, :128]
            natural[2 * field + 1, rows, :] = got[:, 128:]
    for field in range(2):
        for p in range(2):
            for t in range(T):
                kf_ref[2 * field + p, t] = natural[2 * field + p, pl.ds(t, 8, stride=T), :]
    steps = [jnp.broadcast_to(heard[:, j : j + 1], (64, 128)) for j in range(8)]
    n = lane((64, 128))
    pattern = jnp.zeros((64, 128), F32)
    for j in range(8):
        pattern = jnp.where((n >> 4) == j, steps[j], pattern)
    folded = jnp.sum(near_ref[64:128] * pattern, axis=0, keepdims=True)
    folded = jnp.broadcast_to(folded, (8, 128))
    outside = folded
    for j in range(1, 8):
        outside = outside + pltpu.roll(folded, 128 - 16 * j, 1)
    inside = []
    for i in range(3):
        total = jnp.zeros((64, 128), F32)
        for j in range(8):
            total = total + steps[j] * tile[i, pl.ds(j, 64, stride=8), :]
        inside.append(jnp.broadcast_to(jnp.sum(total, axis=0, keepdims=True), (8, 128)))
    n = lane((8, 128))
    low = jnp.where(q == 0, outside, pltpu.roll(inside[0], HALO, 1))
    high = pltpu.roll(jnp.where(q == 3, outside, inside[2]), HALO, 1)
    ends = jnp.where(n < HALO, low, jnp.where(n < 2 * HALO, high, 0.0))
    profile = select_dot(jnp.concatenate([inside[1], ends], axis=1), chosen[0])
    profile = jnp.where(sub((8, 256)) == 0, profile, 0.0)
    begin = []
    for p in range(2):
        k, f = kf_ref[p, 0], kf_ref[2 + p, 0]
        begin.append((k + f) * profile[:, 128 * p : 128 * p + 128] / (4.0 * k + f + SIGMA))
    stencils, work = scratch[:7], scratch[7:]
    build_stencils(kf_ref, stencils, work[4], True)
    result = work[2]

    def finish(t, values):
        for p in range(2):
            result[p, t] = values[p]

    solve_on_slab(
        kf_ref, lambda t: tuple(begin) if t == 0 else None, stencils, work, True, finish
    )
    chosen = from_pairs_matrix()
    both = jnp.concatenate(
        [result[0].reshape(256, 128), result[1].reshape(256, 128)], axis=1
    )
    got = select_dot(both, chosen)
    for t in range(T):
        out_ref[pl.ds(t, 8, stride=T), :] = got[8 * t : 8 * t + 8]


def pack_kernel(slot_ref, in_ref, field_ref, out_ref):
    for q in range(4):
        field_ref[:, 128 * q : 128 * q + 128] = in_ref[q]
    out_ref[...] = jnp.zeros(out_ref.shape, F32)
    for i in range(256):
        r, q = divmod(i, 4)
        out_ref[pl.ds(slot_ref[i], 1), :] = in_ref[q, r : r + 1]


def voxel_kernel(in_ref, heard_ref, weight_ref, spread_ref, response_ref, out_ref):
    p = lane((128, 512))
    spot = jnp.where(sub((128, 512)) == SLOTS + (p & (SLOTS - 1)), 1.0, 0.0).astype(BF)
    rows = jnp.dot(heard_ref[...].astype(BF), spot, preferred_element_type=F32)
    mine = (lane((64, 512)) >> 3) == sub((64, 512))
    rows = jnp.sum(jnp.where(mine, rows, 0.0), axis=0, keepdims=True)
    rows = jnp.broadcast_to(rows, (VROWS, 512))
    mask = jnp.where(rows == sub((VROWS, 512)).astype(F32), 1.0, 0.0)
    chosen = mask.astype(BF)
    voxels = None
    for part in reversed(split3(in_ref[...])):
        got = jnp.dot(chosen, part, preferred_element_type=F32)
        voxels = got if voxels is None else voxels + got
    spread = spread_ref[...]
    response = lax.dot_general(
        voxels, spread, (((1,), (1,)), ((), ())), precision=HIGH, preferred_element_type=F32
    )
    response_ref[...] = response
    weighted = jnp.dot(
        weight_ref[...] * response, spread, precision=HIGH, preferred_element_type=F32
    )
    back = jnp.transpose(mask).astype(BF)
    total = None
    for part in reversed(split3(weighted)):
        got = jnp.dot(back, part, preferred_element_type=F32)
        total = got if total is None else total + got
    n = lane((8, 128))
    width = SLOTS + 2
    blank = jnp.zeros((1, 128), F32)
    out_ref[SLOTS] = blank
    out_ref[width * 63 + SLOTS + 1] = blank
    for u in range(64):
        own = total[SLOTS * u : SLOTS * u + SLOTS]
        for k in range(SLOTS):
            out_ref[width * u + k] = own[k : k + 1]
        if u < 63:
            last = jnp.where(n < HALO, pltpu.roll(own, HALO, 1), 0.0)
            last = pltpu.roll(last, 0, 1, stride=16, stride_axis=0)
            out_ref[width * (u + 1) + SLOTS] = jnp.sum(last, axis=0, keepdims=True)
        if u > 0:
            first = jnp.where(n < HALO, own, 0.0)
            first = pltpu.roll(first, 0, 1, stride=16, stride_axis=0)
            out_ref[width * (u - 1) + SLOTS + 1] = jnp.sum(first, axis=0, keepdims=True)


def driving_kernel(place_ref, slot_ref, near_ref, in_ref, *rest):
    outs, (blocks, ends) = rest[:4], rest[4:]
    for i in range(256):
        r, q = divmod(i, 4)
        at = slot_ref[i]
        blocks[q, r : r + 1] = in_ref[at + 2 * (at >> 3)]
    for side in range(2):
        for r in range(64):
            at = near_ref[side, r]
            row = in_ref[(SLOTS + 2) * (at >> 3) + SLOTS + side]
            turn = (128 - 16 * (at & 7) + HALO * side) & 127
            ends[side, r : r + 1] = pltpu.roll(row, turn, 1)
    n = lane((64, 128))
    for far in range(4):
        q = (place_ref[0] + far) & 3
        low, high = edge_tile(
            blocks[jnp.maximum(q - 1, 0)], blocks[jnp.minimum(q + 1, 3)], HALO
        )
        low = jnp.where(q == 0, jnp.where(n < HALO, ends[0], 0.0), low)
        high = jnp.where(
            q == 3, jnp.where((n >= HALO) & (n < 2 * HALO), ends[1], 0.0), high
        )
        outs[far][0] = blocks[q]
        outs[far][1] = low + high


def stencil_kernel(kf_ref, after_ref, *rest):
    build_stencils(kf_ref, rest[:7], rest[7], False)


def adjoint_kernel(place_ref, tile, kf_ref, *rest):
    slabs, stencils, rest = rest[:4], rest[4:11], rest[11:]
    out_ref, natural, begin, *work = rest
    chosen = to_pairs_matrix(0)
    for far, slab in enumerate(slabs):
        got = select_dot(jnp.concatenate([slab[0], slab[1]], axis=1), chosen)
        rows = pl.ds(pl.multiple_of(64 * ((place_ref[0] - far) & 3), 64), 64)
        natural[0, rows, :] = got[:, :128]
        natural[1, rows, :] = got[:, 128:]
    for p in range(2):
        for t in range(T):
            begin[p, t] = natural[p, pl.ds(t, 8, stride=T), :] * stencils[2][p, t]
    flux = []

    def finish(t, values):
        if t == 0:
            for p in range(2):
                flux.append((kf_ref[p, 0] + kf_ref[2 + p, 0]) * values[p])

    solve_on_slab(
        kf_ref, lambda t: (begin[0, t], begin[1, t]), stencils, work, False, finish
    )
    natural_flux = select_dot(jnp.concatenate(flux, axis=1), from_pairs_matrix())
    row = natural_flux[0:1]
    out = jnp.zeros((256, 128), F32)
    for j in range(2):
        modes = tile[1, pl.ds(j, 256, stride=2), :]
        part = jnp.sum(modes * row, axis=1, keepdims=True)
        out = jnp.where(lane((256, 128)) == j, part, out)
    out_ref[...] = out


VM = pl.BlockSpec(memory_space=pltpu.VMEM)
SM = pl.BlockSpec(memory_space=pltpu.SMEM)
FAR = pl.BlockSpec(memory_space=pltpu.HBM)
PARAMS = pltpu.CompilerParams(vmem_limit_bytes=16 << 20)


def held(*dims, dtype=F32):
    return pltpu.VMEM(dims, dtype)


def run(kernel, name, ins, outs, scratch=(), far=()):
    specs, placed = [], []
    for i, array in enumerate(ins):
        if array.dtype == jnp.int32 and i not in far:
            specs.append(SM)
        elif i in far:
            specs.append(pl.BlockSpec() if i < 6 else FAR)
            array = pltpu.with_memory_space_constraint(array, pltpu.HBM)
        else:
            specs.append(VM)
            array = pltpu.with_memory_space_constraint(array, pltpu.VMEM)
        placed.append(array)
    return pl.pallas_call(
        kernel,
        in_specs=specs,
        out_specs=[VM] * len(outs),
        out_shape=outs,
        scratch_shapes=list(scratch),
        compiler_params=PARAMS,
        name=name,
    )(*placed)


def exchange(array, axis):
    return lax.all_to_all(array, axis, split_axis=0, concat_axis=0, tiled=True)


def on_device(
    diffusivity,
    background_flow,
    inlet_modes,
    profile_step,
    brick_owner,
    voxel_row,
    noise_weight,
    spread_matrix,
):
    count = lax.axis_size("sub")
    place = jnp.stack([lax.axis_index("seg"), lax.axis_index("sub")]).astype(jnp.int32)

    *slab, message, slots, tile = run(
        prepare_kernel,
        "prepare",
        (
            place,
            diffusivity,
            background_flow,
            brick_owner.reshape(1, 256),
            voxel_row.reshape(1, 256),
            profile_step.reshape(1, 8),
            inlet_modes,
        ),
        (held(3, 64, 128),) * 4
        + (held(64, 128), held(1, 256, dtype=jnp.int32), held(3, 512, 128)),
        [pltpu.SemaphoreType.DMA((3,))],
        far=(1, 2, 3, 4, 5, 6),
    )
    slots = slots.reshape(256)
    for far in (2, 1, 3):
        slab[far] = lax.ppermute(slab[far], "seg", [(i, (i + far) % 4) for i in range(4)])
    to_near, message = run(
        border_kernel,
        "border",
        (place, tile, message, *slab),
        (held(128, 128), held(64, 128)),
    )
    outward = [(3 * count + i, i + 1) for i in range(count - 1)]
    outward += [(i + 1, 3 * count + i) for i in range(count - 1)]
    from_near = lax.ppermute(to_near, ALL, outward)
    heard = exchange(message.reshape(count, 1, 128), "sub").reshape(count, 128)

    field, kf, near_slots = run(
        forward_kernel,
        "forward",
        (place, *slab, from_near, heard, tile),
        (held(256, 128), held(4, T, 8, 128), held(2, 128, dtype=jnp.int32)),
        [
            pltpu.VMEM((4, 256, 128), F32),
        ]
        + SOLVE_SCRATCH,
    )
    back = exchange(field.reshape(4, 64, 128), "seg")

    forward_field, packed = run(
        pack_kernel, "pack", (slots, back), (held(64, 512), held(count * SLOTS, 128))
    )
    arrived = exchange(packed.reshape(count, SLOTS, 128), "sub")

    response, answer = run(
        voxel_kernel,
        "voxels",
        (arrived.reshape(count * SLOTS, 128), heard, noise_weight, spread_matrix),
        (held(VROWS, 128), held(count * (SLOTS + 2), 1, 128)),
    )
    answered = exchange(answer, "sub")

    slab = run(
        driving_kernel,
        "driving",
        (place, slots, near_slots, answered),
        (held(2, 64, 128),) * 4,
        [pltpu.VMEM((4, 64, 128), F32), pltpu.VMEM((2, 64, 128), F32)],
    )
    sent = slab[0]
    slab = [sent] + [
        lax.ppermute(slab[far], "seg", [(i, (i + far) % 4) for i in range(4)])
        for far in (1, 2, 3)
    ]
    stencils = run(
        stencil_kernel,
        "stencils",
        (kf, sent),
        tuple(held(*dims) for dims in STENCIL_SHAPES),
        [pltpu.VMEM((1, TC, 8, 128), F32)],
    )

    (partial,) = run(
        adjoint_kernel,
        "adjoint",
        (place, tile, kf, *slab, *stencils),
        (held(256, 128),),
        [
            pltpu.VMEM((2, 256, 128), F32),
            pltpu.VMEM((2, T, 8, 128), F32),
        ]
        + [pltpu.VMEM(dims, F32) for dims in WORK_SHAPES],
    )
    gathered = exchange(partial.reshape(256, 1, 128), ALL)
    product = jnp.sum(gathered, axis=(0, 1))[:2]
    return (forward_field, response, product)


def solution(mesh):
    in_specs = (
        P("seg", "sub"),
        P("seg", "sub"),
        P(None, "sub"),
        P("sub"),
        P(ALL, None),
        P(ALL),
        P(ALL, None),
        P(),
    )
    out_specs = (P("seg", "sub"), P(ALL, None), P(ALL))
    return jax.shard_map(
        on_device, mesh=mesh, in_specs=in_specs, out_specs=out_specs, check_vma=False
    )
```

```python
import jax
import jax.numpy as jnp
from jax import lax
from jax.experimental import pallas as pl
from jax.experimental.pallas import tpu as pltpu
from jax.sharding import PartitionSpec as P

SIGMA = 0.001
HIGH = lax.Precision.HIGHEST
BF = jnp.bfloat16
F32 = jnp.float32
HALO = 12
PAIRS = 76
T = 32
TC = 16
SLOTS = 8
VROWS = 16
ALL = ("seg", "sub")


def split3(x):
    hi = x.astype(BF)
    rest = x - hi.astype(F32)
    mid = rest.astype(BF)
    lo = (rest - mid.astype(F32)).astype(BF)
    return hi, mid, lo


def select_dot(x, chosen):
    hi, mid, lo = split3(x)
    out = jnp.dot(lo, chosen, preferred_element_type=F32)
    out = out + jnp.dot(mid, chosen, preferred_element_type=F32)
    return out + jnp.dot(hi, chosen, preferred_element_type=F32)


def lane(shape):
    return lax.broadcasted_iota(jnp.int32, shape, len(shape) - 1)


def sub(shape):
    return lax.broadcasted_iota(jnp.int32, shape, len(shape) - 2)


def to_pairs_matrix(offset):
    n = lane((256, 256))
    pair = jnp.where(n < 128, n, n - 128)
    x = 2 * pair + jnp.where(n < 128, 0, 1)
    source = jnp.where(
        x < HALO,
        128 + offset + x,
        jnp.where(x < HALO + 128, x - HALO, 128 + offset + x - 128),
    )
    hit = (source == sub((256, 256))) & (pair < PAIRS)
    return jnp.where(hit, 1.0, 0.0).astype(BF)


def from_pairs_matrix():
    row = sub((256, 128))
    y = lane((256, 128))
    source = (y >> 1) + HALO // 2 + jnp.where((y & 1) == 1, 128, 0)
    return jnp.where(source == row, 1.0, 0.0).astype(BF)


def edge_tile(tile_low, tile_high, shift):
    n = lane(tile_low.shape)
    base = shift - HALO
    low = jnp.where((n >= base) & (n < base + HALO), pltpu.roll(tile_low, shift, 1), 0.0)
    high = jnp.where(
        (n >= shift) & (n < shift + HALO), pltpu.roll(tile_high, shift, 1), 0.0
    )
    return low, high


def prepare_kernel(
    place_ref, k_ref, f_ref, owner_ref, row_ref, step_ref, *outs
):
    message_ref, slot_ref = outs[4:]
    owner_row = owner_ref[...]
    owner = jnp.transpose(jnp.broadcast_to(owner_row.astype(F32), (8, 256)))[:, 0:1]
    row = jnp.transpose(jnp.broadcast_to(row_ref[...].astype(F32), (8, 256)))[:, 0:1]
    same = owner == owner_row.astype(F32)
    i, j = sub((256, 256)), lane((256, 256))
    rank = jnp.sum(jnp.where(same & (j < i), 1.0, 0.0), axis=1, keepdims=True)
    rank_row = jnp.sum(jnp.where(same & (i < j), 1.0, 0.0), axis=0, keepdims=True)
    slots = owner_row * SLOTS + rank_row.astype(jnp.int32)
    slot_ref[...] = slots
    held = jnp.where(owner_row == sub((64, 256)), 1.0, 0.0).astype(BF)
    n = lane((256, 128))
    named = jnp.where(n == SLOTS + rank.astype(jnp.int32), row - float(VROWS), 0.0).astype(BF)
    n, m = lane((64, 128)), sub((64, 128))
    message = jnp.dot(held, named, preferred_element_type=F32) + jnp.where(
        (n >= SLOTS) & (n < 2 * SLOTS), float(VROWS), 0.0
    )
    spots = jnp.broadcast_to(slots.astype(F32), (8, 256))
    for q, towards in ((3, 1), (0, -1)):
        chosen = jnp.where(sub((256, 128)) == 4 * (lane((256, 128)) - 64) + q, 1.0, 0.0)
        told = select_dot(spots, chosen.astype(BF))[0:1]
        message = jnp.where((m == place_ref[1] + towards) & (n >= 64), told, message)
    message_ref[...] = message
    message_ref[:, 0:8] = jnp.broadcast_to(step_ref[...], (64, 8))
    for far in range(4):
        q = (place_ref[0] + far) & 3
        own = pl.ds(pl.multiple_of(128 * q, 128), 128)
        below = pl.ds(pl.multiple_of(128 * jnp.maximum(q - 1, 0), 128), 128)
        above = pl.ds(pl.multiple_of(128 * jnp.minimum(q + 1, 3), 128), 128)
        outs[far][0:64] = k_ref[:, own]
        outs[far][64:128] = f_ref[:, own]
        halo = jnp.zeros((64, 128), F32)
        for ref, shift in ((k_ref, HALO), (f_ref, 3 * HALO)):
            low, high = edge_tile(ref[:, below], ref[:, above], shift)
            halo = halo + jnp.where(q > 0, low, 0.0) + jnp.where(q < 3, high, 0.0)
        outs[far][128:160] = halo[0:32] + pltpu.roll(halo[32:64], 64, 1)

def load_kernel(place_ref, modes_ref, after_ref, tile, sems):
    copies = []
    for i in range(3):
        start = 128 * jnp.clip(place_ref[0] + i - 1, 0, 3)
        copies.append(
            pltpu.make_async_copy(
                modes_ref.at[:, pl.ds(pl.multiple_of(start, 128), 128)], tile.at[i], sems.at[i]
            )
        )
        copies[-1].start()
    for copy in copies:
        copy.wait()


def border_kernel(
    place_ref, tile, message_ref, slab_0, slab_1, slab_2, slab_3, out_ref, told_ref
):
    q = place_ref[0]
    told_ref[...] = message_ref[...]
    n = lane((64, 128))
    sent = jnp.zeros((64, 128), F32)
    for far, slab_ref in enumerate((slab_0, slab_1, slab_2, slab_3)):
        k, f = slab_ref[0:64], slab_ref[64:128]
        k = jnp.where(n < HALO, jnp.where(q == 3, pltpu.roll(k, HALO, 1), k), 0.0)
        f = jnp.where(n < HALO, jnp.where(q == 3, pltpu.roll(f, HALO, 1), f), 0.0)
        both = k + pltpu.roll(f, HALO, 1)
        sent = sent + pltpu.roll(both, 2 * HALO * ((q - far) & 3), 1)
    out_ref[0:64] = sent
    sent = jnp.zeros((64, 128), F32)
    for j in range(8):
        x = tile[1, pl.ds(j, 64, stride=8), :]
        x = jnp.where(n < HALO, jnp.where(q == 3, pltpu.roll(x, HALO, 1), x), 0.0)
        sent = sent + (pltpu.roll(x, 16 * j, 1) if j else x)
    out_ref[64:128] = sent


def halo_from(near, g, first):
    n = lane((64, 128))
    x = pltpu.roll(near, (128 - 2 * HALO * g) & 127, 1)
    k = jnp.where(n < HALO, x, 0.0)
    f = jnp.where((n >= HALO) & (n < 2 * HALO), x, 0.0)
    low = k + pltpu.roll(f, HALO, 1)
    return jnp.where(first, low, pltpu.roll(low, HALO, 1))


def shifted(x, amount):
    n = sub(x.shape)
    if amount > 0:
        return jnp.where(n >= amount, pltpu.roll(x, amount, 0), 0.0)
    return jnp.where(n < 8 + amount, pltpu.roll(x, 8 + amount, 0), 0.0)


class Level:
    def __init__(self, gains, prefix, partial, count, forward):
        self.gains, self.prefix, self.partial = gains, prefix, partial
        self.count, self.forward = count, forward
        self.order = range(count) if forward else range(count - 1, -1, -1)

    def multiply(self, parts):
        for p in range(parts):
            running = None
            for t in self.order:
                g = self.gains[p, t]
                running = g if running is None else running * g
                self.prefix[p, t] = running

    def prepare(self, parts):
        one = 1 if self.forward else -1
        self.steps = []
        for p in range(parts):
            a = shifted(self.prefix[p, self.order[-1]], one)
            steps = []
            for d in (1, 2, 4):
                steps.append(a)
                a = a * shifted(a, one * d)
            self.steps.append(steps)

    def scan(self, parts, driving, emit):
        one = 1 if self.forward else -1
        running = [None] * parts
        for t in self.order:
            xs = driving(t)
            for p in range(parts):
                y = xs[p]
                if running[p] is not None:
                    y = self.gains[p, t] * running[p] + y
                running[p] = y
                self.partial[p, t] = y
        carry = []
        for p in range(parts):
            b = shifted(running[p], one)
            for d, a in zip((1, 2, 4), self.steps[p]):
                b = b + a * shifted(b, one * d)
            carry.append(b)
        for t in self.order:
            emit(t, [self.partial[p, t] + self.prefix[p, t] * carry[p] for p in range(parts)])


def beside(ref, t, count, forward, p):
    if forward:
        return ref[p, t + 1] if t + 1 < count else shifted(ref[p, 0], -1)
    return ref[p, t - 1] if t > 0 else shifted(ref[p, count - 1], 1)


def fine_sum(ref, t, forward):
    even, odd = ref[0, t], ref[1, t]
    return (
        beside(ref, t, T, forward, 0) + odd + pltpu.roll(odd, 1, 1),
        beside(ref, t, T, forward, 1) + even + pltpu.roll(even, 127, 1),
    )


def coarse_sum(ref, t, forward):
    own = ref[0, t]
    return beside(ref, t, TC, forward, 0) + pltpu.roll(own, 1, 1) + pltpu.roll(own, 127, 1)


STENCIL_SHAPES = [(2, T, 8, 128)] * 3 + [(1, TC, 8, 128)] * 4
WORK_SHAPES = [(2, T, 8, 128)] * 3 + [(1, TC, 8, 128)] * 3
SOLVE_SCRATCH = [pltpu.VMEM(dims, F32) for dims in STENCIL_SHAPES + WORK_SHAPES]


def build_stencils(kf, stencils, sums, forward):
    gains, prefix, scale, cgains, cprefix, cscale, ck = stencils
    for c in range(TC):
        ksum = fsum = None
        for t in (2 * c, 2 * c + 1):
            for p in range(2):
                k, f = kf[p, t], kf[2 + p, t]
                inverse = 1.0 / (4.0 * k + f + SIGMA)
                if forward:
                    gains[p, t] = (k + f) * inverse
                    scale[p, t] = k * inverse
                else:
                    if t + 1 < T:
                        up = kf[p, t + 1] + kf[2 + p, t + 1]
                    else:
                        up = shifted(kf[p, 0] + kf[2 + p, 0], -1)
                    gains[p, t] = up * inverse
                    scale[p, t] = inverse
                ksum = k if ksum is None else ksum + k
                fsum = f if fsum is None else fsum + f
        kc = 0.25 * ksum
        fc = 0.5 * fsum
        inverse = 1.0 / (4.0 * kc + fc + 4.0 * SIGMA)
        ck[0, c] = kc
        sums[0, c] = kc + fc
        cscale[0, c] = inverse
    for c in range(TC):
        if forward:
            cgains[0, c] = sums[0, c] * cscale[0, c]
        else:
            up = sums[0, c + 1] if c + 1 < TC else shifted(sums[0, 0], -1)
            cgains[0, c] = up * cscale[0, c]
    Level(gains, prefix, None, T, forward).multiply(2)
    Level(cgains, cprefix, None, TC, forward).multiply(1)


def solve_on_slab(kf, source, stencils, work, forward, finish):
    gains, prefix, scale, cgains, cprefix, cscale, ck = stencils
    partial, field, kept, cpartial, cfield, csource = work
    fine = Level(gains, prefix, partial, T, forward)
    fine.prepare(2)
    coarse = Level(cgains, cprefix, cpartial, TC, forward)
    coarse.prepare(1)

    def keep_fine(t, values):
        for p in range(2):
            field[p, t] = values[p] if forward else kf[p, t] * values[p]

    def correct(residual):
        for c in range(TC):
            total = None
            for t in (2 * c, 2 * c + 1):
                for part in residual(t):
                    total = part if total is None else total + part
            csource[0, c] = total * cscale[0, c]

        def keep_first(c, values):
            cfield[0, c] = values[0] if forward else ck[0, c] * values[0]

        coarse.scan(1, lambda c: (csource[0, c],), keep_first)

        def second(c):
            total = coarse_sum(cfield, c, forward)
            if forward:
                total = ck[0, c] * total
            return (csource[0, c] + cscale[0, c] * total,)

        def add_back(c, values):
            for t in (2 * c, 2 * c + 1):
                for p in range(2):
                    more = values[0] if forward else kf[p, t] * values[0]
                    field[p, t] = field[p, t] + more

        coarse.scan(1, second, add_back)

    def relaxed(t):
        sums = fine_sum(field, t, forward)
        start = source(t)
        return tuple(
            scale[p, t] * sums[p] if start is None else start[p] + scale[p, t] * sums[p]
            for p in range(2)
        )

    def started(t):
        start = source(t)
        return (jnp.zeros((8, 128), F32),) * 2 if start is None else start

    def residual_first(t):
        sums = fine_sum(field, t, forward)
        return tuple(kf[p, t] * sums[p] if forward else sums[p] for p in range(2))

    def relaxed_kept(t):
        sums = fine_sum(field, t, forward)
        start = source(t)
        for p in range(2):
            kept[p, t] = sums[p]
        return tuple(
            scale[p, t] * sums[p] if start is None else start[p] + scale[p, t] * sums[p]
            for p in range(2)
        )

    def residual_second(t):
        sums = fine_sum(field, t, forward)
        parts = tuple(sums[p] - kept[p, t] for p in range(2))
        return tuple(kf[p, t] * parts[p] if forward else parts[p] for p in range(2))

    fine.scan(2, started, keep_fine)
    correct(residual_first)
    fine.scan(2, relaxed, keep_fine)
    fine.scan(2, relaxed_kept, keep_fine)
    correct(residual_second)
    fine.scan(2, relaxed, finish)


def forward_kernel(
    place_ref, slab_0, slab_1, slab_2, slab_3, near_ref, heard_ref, tile,
    out_ref, kf_ref, slot_ref, natural, *scratch,
):
    heard = heard_ref[...]
    for side, other in enumerate((place_ref[1] - 1, place_ref[1] + 1)):
        told = jnp.sum(jnp.where(sub((64, 128)) == other, heard, 0.0), axis=0, keepdims=True)
        slot_ref[side : side + 1] = pltpu.roll(told, 64, 1).astype(jnp.int32)
    q = place_ref[0]
    outer = near_ref[0:64]
    chosen = [to_pairs_matrix(2 * HALO * field) for field in range(2)]
    for far, slab_ref in enumerate((slab_0, slab_1, slab_2, slab_3)):
        g = (q - far) & 3
        halo = slab_ref[128:160]
        halo = jnp.concatenate([halo, pltpu.roll(halo, 64, 1)], axis=0)
        halo = jnp.where(lane((64, 128)) < 4 * HALO, halo, 0.0) + halo_from(outer, g, q == 0)
        rows = pl.ds(pl.multiple_of(64 * g, 64), 64)
        for field in range(2):
            x = jnp.concatenate([slab_ref[64 * field : 64 * field + 64], halo], axis=1)
            got = select_dot(x, chosen[field])
            natural[2 * field, rows, :] = got[:, :128]
            natural[2 * field + 1, rows, :] = got[:, 128:]
    for field in range(2):
        for p in range(2):
            for t in range(T):
                kf_ref[2 * field + p, t] = natural[2 * field + p, pl.ds(t, 8, stride=T), :]
    steps = [jnp.broadcast_to(heard[:, j : j + 1], (64, 128)) for j in range(8)]
    n = lane((64, 128))
    pattern = jnp.zeros((64, 128), F32)
    for j in range(8):
        pattern = jnp.where((n >> 4) == j, steps[j], pattern)
    folded = jnp.sum(near_ref[64:128] * pattern, axis=0, keepdims=True)
    folded = jnp.broadcast_to(folded, (8, 128))
    outside = folded
    for j in range(1, 8):
        outside = outside + pltpu.roll(folded, 128 - 16 * j, 1)
    inside = []
    for i in range(3):
        total = jnp.zeros((64, 128), F32)
        for j in range(8):
            total = total + steps[j] * tile[i, pl.ds(j, 64, stride=8), :]
        inside.append(jnp.broadcast_to(jnp.sum(total, axis=0, keepdims=True), (8, 128)))
    n = lane((8, 128))
    low = jnp.where(q == 0, outside, pltpu.roll(inside[0], HALO, 1))
    high = pltpu.roll(jnp.where(q == 3, outside, inside[2]), HALO, 1)
    ends = jnp.where(n < HALO, low, jnp.where(n < 2 * HALO, high, 0.0))
    profile = select_dot(jnp.concatenate([inside[1], ends], axis=1), chosen[0])
    profile = jnp.where(sub((8, 256)) == 0, profile, 0.0)
    begin = []
    for p in range(2):
        k, f = kf_ref[p, 0], kf_ref[2 + p, 0]
        begin.append((k + f) * profile[:, 128 * p : 128 * p + 128] / (4.0 * k + f + SIGMA))
    stencils, work = scratch[:7], scratch[7:]
    build_stencils(kf_ref, stencils, work[4], True)
    result = work[2]

    def finish(t, values):
        for p in range(2):
            result[p, t] = values[p]

    solve_on_slab(
        kf_ref, lambda t: tuple(begin) if t == 0 else None, stencils, work, True, finish
    )
    chosen = from_pairs_matrix()
    both = jnp.concatenate(
        [result[0].reshape(256, 128), result[1].reshape(256, 128)], axis=1
    )
    got = select_dot(both, chosen)
    for t in range(T):
        out_ref[pl.ds(t, 8, stride=T), :] = got[8 * t : 8 * t + 8]


def pack_kernel(slot_ref, in_ref, field_ref, out_ref):
    for q in range(4):
        field_ref[:, 128 * q : 128 * q + 128] = in_ref[q]
    out_ref[...] = jnp.zeros(out_ref.shape, F32)
    for i in range(256):
        r, q = divmod(i, 4)
        out_ref[pl.ds(slot_ref[i], 1), :] = in_ref[q, r : r + 1]


def voxel_kernel(in_ref, heard_ref, weight_ref, spread_ref, response_ref, out_ref):
    p = lane((128, 512))
    spot = jnp.where(sub((128, 512)) == SLOTS + (p & (SLOTS - 1)), 1.0, 0.0).astype(BF)
    rows = jnp.dot(heard_ref[...].astype(BF), spot, preferred_element_type=F32)
    mine = (lane((64, 512)) >> 3) == sub((64, 512))
    rows = jnp.sum(jnp.where(mine, rows, 0.0), axis=0, keepdims=True)
    rows = jnp.broadcast_to(rows, (VROWS, 512))
    mask = jnp.where(rows == sub((VROWS, 512)).astype(F32), 1.0, 0.0)
    chosen = mask.astype(BF)
    voxels = None
    for part in reversed(split3(in_ref[...])):
        got = jnp.dot(chosen, part, preferred_element_type=F32)
        voxels = got if voxels is None else voxels + got
    spread = spread_ref[...]
    response = lax.dot_general(
        voxels, spread, (((1,), (1,)), ((), ())), precision=HIGH, preferred_element_type=F32
    )
    response_ref[...] = response
    weighted = jnp.dot(
        weight_ref[...] * response, spread, precision=HIGH, preferred_element_type=F32
    )
    back = jnp.transpose(mask).astype(BF)
    total = None
    for part in reversed(split3(weighted)):
        got = jnp.dot(back, part, preferred_element_type=F32)
        total = got if total is None else total + got
    n = lane((8, 128))
    width = SLOTS + 2
    blank = jnp.zeros((1, 128), F32)
    out_ref[SLOTS] = blank
    out_ref[width * 63 + SLOTS + 1] = blank
    for u in range(64):
        own = total[SLOTS * u : SLOTS * u + SLOTS]
        for k in range(SLOTS):
            out_ref[width * u + k] = own[k : k + 1]
        if u < 63:
            last = jnp.where(n < HALO, pltpu.roll(own, HALO, 1), 0.0)
            last = pltpu.roll(last, 0, 1, stride=16, stride_axis=0)
            out_ref[width * (u + 1) + SLOTS] = jnp.sum(last, axis=0, keepdims=True)
        if u > 0:
            first = jnp.where(n < HALO, own, 0.0)
            first = pltpu.roll(first, 0, 1, stride=16, stride_axis=0)
            out_ref[width * (u - 1) + SLOTS + 1] = jnp.sum(first, axis=0, keepdims=True)


def driving_kernel(place_ref, slot_ref, near_ref, in_ref, *rest):
    outs, (blocks, ends) = rest[:4], rest[4:]
    for i in range(256):
        r, q = divmod(i, 4)
        at = slot_ref[i]
        blocks[q, r : r + 1] = in_ref[at + 2 * (at >> 3)]
    for side in range(2):
        for r in range(64):
            at = near_ref[side, r]
            row = in_ref[(SLOTS + 2) * (at >> 3) + SLOTS + side]
            turn = (128 - 16 * (at & 7) + HALO * side) & 127
            ends[side, r : r + 1] = pltpu.roll(row, turn, 1)
    n = lane((64, 128))
    for far in range(4):
        q = (place_ref[0] + far) & 3
        low, high = edge_tile(
            blocks[jnp.maximum(q - 1, 0)], blocks[jnp.minimum(q + 1, 3)], HALO
        )
        low = jnp.where(q == 0, jnp.where(n < HALO, ends[0], 0.0), low)
        high = jnp.where(
            q == 3, jnp.where((n >= HALO) & (n < 2 * HALO), ends[1], 0.0), high
        )
        outs[far][0:64] = blocks[q]
        halo = low + high
        packed = halo[0:16]
        for g in range(1, 4):
            packed = packed + pltpu.roll(halo[16 * g : 16 * g + 16], 32 * g, 1)
        outs[far][64:80] = packed


def stencil_kernel(kf_ref, after_ref, *rest):
    build_stencils(kf_ref, rest[:7], rest[7], False)


def adjoint_kernel(place_ref, tile, kf_ref, *rest):
    slabs, stencils, rest = rest[:4], rest[4:11], rest[11:]
    out_ref, natural, begin, *work = rest
    chosen = to_pairs_matrix(0)
    for far, slab in enumerate(slabs):
        packed = slab[64:80]
        halo = [packed] + [pltpu.roll(packed, 128 - 32 * g, 1) for g in range(1, 4)]
        halo = jnp.concatenate(halo, axis=0)
        got = select_dot(jnp.concatenate([slab[0:64], halo], axis=1), chosen)
        rows = pl.ds(pl.multiple_of(64 * ((place_ref[0] - far) & 3), 64), 64)
        natural[0, rows, :] = got[:, :128]
        natural[1, rows, :] = got[:, 128:]
    for p in range(2):
        for t in range(T):
            begin[p, t] = natural[p, pl.ds(t, 8, stride=T), :] * stencils[2][p, t]
    flux = []

    def finish(t, values):
        if t == 0:
            for p in range(2):
                flux.append((kf_ref[p, 0] + kf_ref[2 + p, 0]) * values[p])

    solve_on_slab(
        kf_ref, lambda t: (begin[0, t], begin[1, t]), stencils, work, False, finish
    )
    natural_flux = select_dot(jnp.concatenate(flux, axis=1), from_pairs_matrix())
    row = natural_flux[0:1]
    out = jnp.zeros((256, 128), F32)
    for j in range(2):
        modes = tile[1, pl.ds(j, 256, stride=2), :]
        part = jnp.sum(modes * row, axis=1, keepdims=True)
        out = jnp.where(lane((256, 128)) == j, part, out)
    out_ref[...] = out


def total_kernel(in_ref, out_ref):
    out_ref[...] = jnp.sum(in_ref[...], axis=0, keepdims=True)[:, 0:2]


VM = pl.BlockSpec(memory_space=pltpu.VMEM)
SM = pl.BlockSpec(memory_space=pltpu.SMEM)
FAR = pl.BlockSpec(memory_space=pltpu.HBM)
PARAMS = pltpu.CompilerParams(vmem_limit_bytes=16 << 20)


def held(*dims, dtype=F32):
    return pltpu.VMEM(dims, dtype)


def run(kernel, name, ins, outs, scratch=(), far=()):
    specs, placed = [], []
    for i, array in enumerate(ins):
        if array.dtype == jnp.int32 and i not in far:
            specs.append(SM)
        elif i in far:
            specs.append(pl.BlockSpec() if name == "prepare" else FAR)
            array = pltpu.with_memory_space_constraint(array, pltpu.HBM)
        else:
            specs.append(VM)
            array = pltpu.with_memory_space_constraint(array, pltpu.VMEM)
        placed.append(array)
    return pl.pallas_call(
        kernel,
        in_specs=specs,
        out_specs=[pl.BlockSpec() if name == "total" else VM] * len(outs),
        out_shape=outs,
        scratch_shapes=list(scratch),
        compiler_params=PARAMS,
        name=name,
    )(*placed)


def exchange(array, axis):
    return lax.all_to_all(array, axis, split_axis=0, concat_axis=0, tiled=True)


def on_device(
    diffusivity,
    background_flow,
    inlet_modes,
    profile_step,
    brick_owner,
    voxel_row,
    noise_weight,
    spread_matrix,
):
    count = lax.axis_size("sub")
    place = jnp.stack([lax.axis_index("seg"), lax.axis_index("sub")]).astype(jnp.int32)

    *slab, message, slots = run(
        prepare_kernel,
        "prepare",
        (
            place,
            diffusivity,
            background_flow,
            brick_owner.reshape(1, 256),
            voxel_row.reshape(1, 256),
            profile_step.reshape(1, 8),
        ),
        (held(160, 128),) * 4 + (held(64, 128), held(1, 256, dtype=jnp.int32)),
        far=(1, 2, 3, 4, 5),
    )
    slots = slots.reshape(256)
    (tile,) = run(
        load_kernel,
        "load",
        (place, inlet_modes, slab[0]),
        (held(3, 512, 128),),
        [pltpu.SemaphoreType.DMA((3,))],
        far=(1,),
    )
    for far in (2, 1, 3):
        slab[far] = lax.ppermute(slab[far], "seg", [(i, (i + far) % 4) for i in range(4)])
    to_near, message = run(
        border_kernel,
        "border",
        (place, tile, message, *slab),
        (held(128, 128), held(64, 128)),
    )
    outward = [(3 * count + i, i + 1) for i in range(count - 1)]
    outward += [(i + 1, 3 * count + i) for i in range(count - 1)]
    from_near = lax.ppermute(to_near, ALL, outward)
    heard = exchange(message.reshape(count, 1, 128), "sub").reshape(count, 128)

    field, kf, near_slots = run(
        forward_kernel,
        "forward",
        (place, *slab, from_near, heard, tile),
        (held(256, 128), held(4, T, 8, 128), held(2, 128, dtype=jnp.int32)),
        [
            pltpu.VMEM((4, 256, 128), F32),
        ]
        + SOLVE_SCRATCH,
    )
    back = exchange(field.reshape(4, 64, 128), "seg")

    forward_field, packed = run(
        pack_kernel, "pack", (slots, back), (held(64, 512), held(count * SLOTS, 128))
    )
    arrived = exchange(packed.reshape(count, SLOTS, 128), "sub")

    response, answer = run(
        voxel_kernel,
        "voxels",
        (arrived.reshape(count * SLOTS, 128), heard, noise_weight, spread_matrix),
        (held(VROWS, 128), held(count * (SLOTS + 2), 1, 128)),
    )
    answered = exchange(answer, "sub")

    slab = run(
        driving_kernel,
        "driving",
        (place, slots, near_slots, answered),
        (held(80, 128),) * 4,
        [pltpu.VMEM((4, 64, 128), F32), pltpu.VMEM((2, 64, 128), F32)],
    )
    sent = slab[0]
    slab = [sent] + [
        lax.ppermute(slab[far], "seg", [(i, (i + far) % 4) for i in range(4)])
        for far in (1, 2, 3)
    ]
    stencils = run(
        stencil_kernel,
        "stencils",
        (kf, sent),
        tuple(held(*dims) for dims in STENCIL_SHAPES),
        [pltpu.VMEM((1, TC, 8, 128), F32)],
    )

    (partial,) = run(
        adjoint_kernel,
        "adjoint",
        (place, tile, kf, *slab, *stencils),
        (held(256, 128),),
        [
            pltpu.VMEM((2, 256, 128), F32),
            pltpu.VMEM((2, T, 8, 128), F32),
        ]
        + [pltpu.VMEM(dims, F32) for dims in WORK_SHAPES],
    )
    gathered = exchange(partial.reshape(256, 1, 128), ALL)
    (product,) = run(
        total_kernel, "total", (gathered.reshape(256, 128),), (jax.ShapeDtypeStruct((1, 2), F32),)
    )
    product = product.reshape(2)
    return (forward_field, response, product)


def solution(mesh):
    in_specs = (
        P("seg", "sub"),
        P("seg", "sub"),
        P(None, "sub"),
        P("sub"),
        P(ALL, None),
        P(ALL),
        P(ALL, None),
        P(),
    )
    out_specs = (P("seg", "sub"), P(ALL, None), P(ALL))
    return jax.shard_map(
        on_device, mesh=mesh, in_specs=in_specs, out_specs=out_specs, check_vma=False
    )
```
